128 devices in a mesh: trees: 1, data: 128 (over z, y, x, core).
Axes of the slice: x: 4, y: 4, z: 4, core: 2. Of those that a mesh axis runs over, the one named last changes fastest.
Arguments:
- bin_codes: int32 [65536, 3072], P(('trees', 'data'))
- gradient: float32 [65536], P(('trees', 'data'))
- hessian: float32 [65536], P(('trees', 'data'))
- valid_rows: int32 [128], P(('trees', 'data'))
- split_feat: int32 [31], P('trees')
- split_thr: int32 [31], P('trees')
- cut_values: float32 [3072, 15], P('trees')
- reg_lambda: float32 [1], P('trees')
Outputs:
- output 1: float32 [63, 3072, 15], P(None, ('trees', 'data'))
- output 2: float32 [32], P('trees')
- output 3: float32 [31], P('trees')
All inputs are finite; a program needn't handle non-finite values.
Results may differ from the reference program's by a relative error of at most 0.001.
Values sent between devices are 32-bit elements.
A program may use at most 1 GiB of HBM per device.

```python
import jax
import jax.numpy as jnp
from jax import lax

ROWS_DEV = 512
GROUP = 128
FEATS = 3072
BINS = 16
DEPTH = 6

ROWS = ROWS_DEV * GROUP
LEAVES = 2 ** (DEPTH - 1)
INNER = LEAVES - 1


def setup_inputs(seed: int = 0, part: int = 0) -> dict:
    base_key = jax.random.fold_in(jax.random.key(seed), part)
    keys = jax.random.split(base_key, 10)
    bin_codes = jax.random.randint(keys[0], (ROWS, FEATS), 0, BINS, dtype=jnp.int32)
    weights = jax.random.normal(keys[1], (FEATS,), jnp.float32) * FEATS ** -0.5
    centred = bin_codes.astype(jnp.float32) / BINS - 0.5
    gradient = 0.4 + 0.8 * jax.random.normal(keys[2], (ROWS,), jnp.float32) + 1.5 * jnp.dot(centred, weights)
    hessian = jax.random.uniform(keys[3], (ROWS,), jnp.float32, 0.2, 1.0)
    counts = jax.random.randint(keys[4], (GROUP,), ROWS_DEV // 16, ROWS_DEV + 1, dtype=jnp.int32)
    device_order = jax.random.permutation(keys[5], GROUP)
    valid_rows = counts.at[device_order[0]].set(ROWS_DEV).at[device_order[1]].set(ROWS_DEV // 16)
    split_feat = jax.random.randint(keys[6], (INNER,), 0, FEATS, dtype=jnp.int32)
    split_thr = jax.random.randint(keys[7], (INNER,), BINS // 8, BINS - BINS // 8, dtype=jnp.int32)
    cut_steps = jax.random.uniform(keys[8], (FEATS, BINS - 1), jnp.float32, 0.5, 1.5)
    cut_values = jnp.cumsum(cut_steps, axis=1) / BINS - 0.5
    reg_lambda = (0.5 + jax.random.uniform(keys[9], (1,), jnp.float32)) * (0.5 * ROWS / LEAVES)
    return {'bin_codes': bin_codes, 'gradient': gradient, 'hessian': hessian, 'valid_rows': valid_rows, 'split_feat': split_feat, 'split_thr': split_thr, 'cut_values': cut_values, 'reg_lambda': reg_lambda}


def level_hist(bin_codes, node_ids, grad_pairs, level_width):
    feat_ids = jnp.arange(FEATS, dtype=jnp.int32)
    cell_count = level_width * FEATS * BINS

    def add_shard(hist_acc, shard_data):
        shard_codes, shard_nodes, shard_pairs = shard_data
        cell_ids = (shard_nodes[:, None] * FEATS + feat_ids[None, :]) * BINS + shard_codes
        values = jnp.broadcast_to(shard_pairs[:, None, :], (ROWS_DEV, FEATS, 2))
        added = jax.ops.segment_sum(values.reshape(ROWS_DEV * FEATS, 2), cell_ids.reshape(ROWS_DEV * FEATS), num_segments=cell_count)
        return hist_acc + added, None

    hist_zero = jnp.zeros((cell_count, 2), jnp.float32)
    histogram, _ = lax.scan(add_shard, hist_zero, (bin_codes.reshape(GROUP, ROWS_DEV, FEATS), node_ids.reshape(GROUP, ROWS_DEV), grad_pairs.reshape(GROUP, ROWS_DEV, 2)))
    return histogram.reshape(level_width, FEATS, BINS, 2)


def level_gains(histogram, reg_lambda):
    prefix = jnp.cumsum(histogram, axis=2)
    left_sum = prefix[:, :, : BINS - 1, :]
    node_sum = prefix[:, :, BINS - 1 :, :]
    right_sum = node_sum - left_sum

    def split_score(pair_sum):
        return pair_sum[..., 0] * pair_sum[..., 0] / (pair_sum[..., 1] + reg_lambda[0])

    return 0.5 * (split_score(left_sum) + split_score(right_sum) - split_score(node_sum))


def reference(bin_codes, gradient, hessian, valid_rows, split_feat, split_thr, cut_values, reg_lambda):
    row_ids = jnp.arange(ROWS, dtype=jnp.int32)
    live_rows = (row_ids % ROWS_DEV) < valid_rows[row_ids // ROWS_DEV]
    grad_pairs = jnp.where(live_rows[:, None], jnp.stack([gradient, hessian], axis=1), 0.0)
    node_ids = jnp.zeros((ROWS,), jnp.int32)
    gain_levels = []
    for level in range(DEPTH):
        level_width = 2 ** level
        gain_levels.append(level_gains(level_hist(bin_codes, node_ids, grad_pairs, level_width), reg_lambda))
        if level < DEPTH - 1:
            heap_ids = level_width - 1 + node_ids
            chosen = jnp.take_along_axis(bin_codes, split_feat[heap_ids][:, None], axis=1)[:, 0]
            node_ids = 2 * node_ids + (chosen > split_thr[heap_ids]).astype(jnp.int32)
    leaf_sum = jax.ops.segment_sum(grad_pairs, node_ids, num_segments=LEAVES)
    leaf_value = -leaf_sum[:, 0] / (leaf_sum[:, 1] + reg_lambda[0])
    split_value = cut_values[split_feat, split_thr]
    return (jnp.concatenate(gain_levels, axis=0), leaf_value, split_value)
```

```python
import math
import jax
import jax.numpy as jnp
from jax import lax
from jax.sharding import PartitionSpec as P


def route(codes, split_feat, split_thr, depth):
    columns = codes[:, split_feat]
    goes_right = columns > split_thr[None, :]
    node = jnp.zeros((codes.shape[0],), jnp.int32)
    inner = jnp.arange(split_feat.shape[0], dtype=jnp.int32)
    heap = node
    for _ in range(depth - 1):
        bit = jnp.any((heap[:, None] == inner[None, :]) & goes_right, axis=1)
        heap = 2 * heap + 1 + bit.astype(jnp.int32)
    return heap - (2 ** (depth - 1) - 1)


def solution(mesh):
    groups = mesh.shape['data']
    row_spec = P(('trees', 'data'))

    def device_fn(bin_codes, gradient, hessian, valid_rows, split_feat, split_thr, cut_values, reg_lambda):
        row_count, feat_count = bin_codes.shape
        bin_count = cut_values.shape[1] + 1
        depth = int(math.log2(split_feat.shape[0] + 1)) + 1
        leaves = 2 ** (depth - 1)
        reg_value = reg_lambda[0]
        live_rows = jnp.arange(row_count, dtype=jnp.int32) < valid_rows[0]
        leaf = route(bin_codes, split_feat, split_thr, depth)
        pairs = jnp.where(live_rows[:, None], jnp.stack([gradient, hessian], axis=1), 0.0)
        in_leaf = leaf[:, None] == jnp.arange(leaves, dtype=jnp.int32)[None, :]
        weighted = jnp.where(in_leaf[:, None, :], pairs[:, :, None], 0.0).reshape(row_count, 2 * leaves)
        bins = jnp.arange(bin_count, dtype=jnp.int32)
        below = (bin_codes[:, None, :] <= bins[None, :, None]).astype(jnp.float32)
        part = jnp.einsum('im,ibf->fbm', weighted, below, preferred_element_type=jnp.float32, precision=lax.Precision.HIGHEST)
        own = lax.psum_scatter(part, 'data', scatter_dimension=0, tiled=True)
        own = own.reshape(own.shape[0], bin_count, 2, leaves)
        levels = [own]
        for _ in range(depth - 1):
            last = levels[0]
            levels.insert(0, last.reshape(last.shape[:-1] + (last.shape[-1] // 2, 2)).sum(-1))
        sums = jnp.concatenate(levels, axis=-1)
        left = sums[:, :bin_count - 1]
        total = sums[:, bin_count - 1:]
        right = total - left

        def score(v):
            return v[:, :, 0] * v[:, :, 0] / (v[:, :, 1] + reg_value)

        gain = 0.5 * (score(left) + score(right) - score(total))
        leaf_sum = own[0, bin_count - 1]
        leaf_value = -leaf_sum[0] / (leaf_sum[1] + reg_value)
        split_value = cut_values[split_feat, split_thr]
        return jnp.transpose(gain, (2, 0, 1)), leaf_value, split_value

    return jax.shard_map(device_fn, mesh=mesh, in_specs=(P(('trees', 'data'), None), row_spec, row_spec, row_spec, P('trees'), P('trees'), P('trees', None), P('trees')), out_specs=(P(None, ('trees', 'data'), None), P('trees'), P('trees')), check_vma=False)
```

```python
import functools
import jax
import jax.numpy as jnp
from jax import lax
from jax.experimental import pallas as pl
from jax.experimental.pallas import tpu as pltpu
from jax.sharding import PartitionSpec as P

F32 = jnp.float32
BF16 = jnp.bfloat16
ROWS = 512
FEATS = 3072
BINS = 16
LEAVES = 32
INNER = 31
LOADS = 8
SLAB = FEATS // LOADS


def pow4(dim):
    return 1 + 3 * dim * (3 * dim - 1) // 2


def coord(me, dim):
    return (me // 2) // pow4(dim) % 4


def neighbour(me, dim, step):
    at = coord(me, dim)
    return me + ((at + step + 4) % 4 - at) * 2 * pow4(dim)


def hist_kernel(codes_hbm, grad_ref, hess_ref, valid_ref, feat_ref, thr_ref, out_ref,
                raw, turned, turned_rx, codes2, meta, weights, hist, rx1, rx2, rx3,
                load_sem, pair_send, pair_recv, send_sem, recv_sem):
    me = lax.axis_index('data')
    core = me % 2
    partner = me + 1 - 2 * core

    def remote(src, dst, s_sem, r_sem, device):
        return pltpu.make_async_remote_copy(src_ref=src, dst_ref=dst, send_sem=s_sem, recv_sem=r_sem, device_id=(0, device), device_id_type=pl.DeviceIdType.MESH)

    barrier = pltpu.get_barrier_semaphore()
    pl.semaphore_signal(barrier, inc=1, device_id=(0, partner), device_id_type=pl.DeviceIdType.MESH)
    for dim in range(3):
        for step in (1, -1):
            pl.semaphore_signal(barrier, inc=1, device_id=(0, neighbour(me, dim, step)), device_id_type=pl.DeviceIdType.MESH)

    def load(m):
        return pltpu.make_async_copy(codes_hbm.at[:, pl.ds(m * SLAB, SLAB)], raw.at[m], load_sem.at[m])

    for m in range(LOADS):
        load(m).start()
    pl.semaphore_wait(barrier, 7)

    def pair_copy(m):
        return remote(turned.at[pl.ds(m * 8, 8), 1 - core], turned_rx.at[pl.ds(m * 8, 8)], pair_send.at[m], pair_recv.at[m], partner)

    meta_copy = remote(meta.at[0], meta.at[1], pair_send.at[LOADS], pair_recv.at[LOADS], partner)

    @pl.loop(0, LOADS)
    def _(m):
        pltpu.make_async_copy(codes_hbm.at[:, pl.ds(0, SLAB)], raw.at[m], load_sem.at[m]).wait()
        block = raw[m].astype(F32)
        turned[pl.ds(m * 8, 8)] = block.T.reshape(8, 2, 24, ROWS)
        pair_copy(m).start()

    def goes_right(j):
        feat = feat_ref[j]
        column = turned[feat // 48, feat // 24 % 2, pl.ds(feat % 24, 1), :]
        return (column > thr_ref[j].astype(F32)).astype(jnp.int32)

    leaf = goes_right(0)
    for level in range(1, 5):
        width = 2 ** level
        bit = goes_right(width - 1)
        for n in range(1, width):
            bit = jnp.where(leaf == n, goes_right(width - 1 + n), bit)
        leaf = 2 * leaf + bit
    live = lax.broadcasted_iota(jnp.int32, (1, ROWS), 1) < valid_ref[0]
    grad = jnp.where(live, grad_ref[...], 0.0)
    hess = jnp.where(live, hess_ref[...], 0.0)
    meta[0] = jnp.concatenate([grad, hess, leaf.astype(F32), jnp.zeros((5, ROWS), F32)], axis=0)
    meta_copy.start()

    def split3(v):
        hi = v.astype(BF16).astype(F32)
        mid = (v - hi).astype(BF16).astype(F32)
        return hi, mid, v - hi - mid

    def fill_weights(side):
        for k in range(ROWS // 128):
            lanes = pl.ds(k * 128, 128)
            g3 = split3(meta[side, 0:1, lanes])
            h3 = split3(meta[side, 1:2, lanes])
            hit = meta[side, 2:3, lanes] == lax.broadcasted_iota(jnp.int32, (LEAVES, 128), 0).astype(F32)
            rows = []
            for i in range(3):
                rows.append(jnp.where(hit, g3[i], 0.0))
                rows.append(jnp.where(hit, h3[i], 0.0))
            rows.append(jnp.zeros((64, 128), F32))
            weights[pl.ds(side * ROWS + k * 128, 128), :] = jnp.concatenate(rows, axis=0).T.astype(BF16)

    fill_weights(0)

    def fill_codes(source, lane0, chip):
        where = (chip % 4, chip // 4 % 4, chip // 16)
        for p in range(3):
            v = source(p)
            codes2[p, where[p], where[(p + 1) % 3], where[(p + 2) % 3], :, pl.ds(lane0, ROWS)] = jnp.concatenate([v, v - 1.0], axis=0).astype(BF16)

    @pl.loop(0, 64, unroll=4)
    def _(chip):
        fill_codes(lambda p: turned[chip, core, pl.ds(8 * p, 8), :], 0, chip)

    meta_copy.wait_recv()
    fill_weights(1)

    @pl.loop(0, LOADS)
    def _(m):
        pair_copy(m).wait_recv()
        for k in range(8):
            chip = m * 8 + k
            fill_codes(lambda p: turned_rx[chip, pl.ds(8 * p, 8), :], ROWS, chip)

    def block(ph, c, p, half, j):
        if ph == 0:
            return hist.at[p, c, j, half]
        ia = coord(me, p)
        if ph == 1:
            return hist.at[p, c, ia, half, j]
        return hist.at[p, c, ia, half, coord(me, (p + 1) % 3), pl.ds(2 * j, 2)]

    def landing(ph, c, p, kind, half):
        return (rx1, rx2, rx3)[ph].at[p, c, kind, half]

    def copy(ph, c, p, kind, half):
        dim = (p + ph) % 3
        at = coord(me, dim)
        step = 1 if (kind == 1) == (half == 1) else -1
        j = (at + 2) % 4 if kind == 0 else (at + step + 4) % 4
        s = ((ph * 2 + c) * 3 + p) * 6 + kind * 2 + half
        return remote(block(ph, c, p, half, j), landing(ph, c, p, kind, half), send_sem.at[s], recv_sem.at[s], neighbour(me, dim, step))

    def send_far(ph, c, p):
        copy(ph, c, p, 0, 0).start()
        copy(ph, c, p, 0, 1).start()

    def send_near(ph, c, p):
        copy(ph, c, p, 1, 1).start()
        copy(ph, c, p, 1, 0).start()

    def relay(ph, c, p):
        at = coord(me, (p + ph) % 3)
        for half in range(2):
            copy(ph, c, p, 0, half).wait_recv()
            mine = block(ph, c, p, half, (at + (1, 3)[half]) % 4)
            mine[...] = mine[...] + landing(ph, c, p, 0, half)[...]
            copy(ph, c, p, 2, half).start()

    def collect(ph, c, p):
        at = coord(me, (p + ph) % 3)
        for half in range(2):
            copy(ph, c, p, 1, half).wait_recv()
            copy(ph, c, p, 2, half).wait_recv()
            mine = block(ph, c, p, half, at)
            mine[...] = mine[...] + landing(ph, c, p, 1, half)[...] + landing(ph, c, p, 2, half)[...]

    def collect_and_send(ph, c, p):
        collect(ph, c, p)
        send_far(ph + 1, c, p)
        send_near(ph + 1, c, p)

    first_half = lax.broadcasted_iota(jnp.int32, (64, 8, 128), 2) < 64

    def unit(c, p, ja):
        pieces = []
        for half in range(2):
            for jb in range(4):
                for jc in range(4):
                    code = codes2[p, ja, jb, jc]
                    for q in range(2):
                        bound = 2.0 * (c * 4 + half * 2 + q)
                        pieces.append(jnp.where(code <= jnp.asarray(bound, BF16), jnp.asarray(1, BF16), jnp.asarray(0, BF16)))
        left = jnp.concatenate(pieces, axis=0)
        sums = jnp.dot(left, weights[...], preferred_element_type=F32)
        sums = (sums[:, :128] + sums[:, 128:]).reshape(64, 2, 8, 128)
        even, odd = sums[:, 0], sums[:, 1]
        keep = jnp.where(first_half, even, odd)
        turn = jnp.where(first_half, odd, even).reshape(512, 128)
        both = keep + pltpu.roll(turn, 64, 1).reshape(64, 8, 128)
        hist[p, c, ja] = both.reshape(2, 4, 8, 8, 128)

    for c in range(2):
        @pl.loop(0, 12)
        def _(u):
            p, jj = u % 3, u // 3
            ahead = (2 + 3 * jj + (jj // 2) * (7 - 2 * jj)) % 4
            unit(c, p, (coord(me, p) + ahead) % 4)

            @pl.when(jj == 0)
            def _():
                send_far(0, c, p)

            @pl.when(jj == 1)
            def _():
                copy(0, c, p, 1, 1).start()

            @pl.when(jj == 2)
            def _():
                copy(0, c, p, 1, 0).start()
                if c == 1:
                    collect_and_send(0, 0, p)

            @pl.when(jj == 3)
            def _():
                if c == 1:
                    relay(1, 0, p)
                relay(0, c, p)

    def for_parts(task):
        @pl.loop(0, 3)
        def _(p):
            task(p)

    for_parts(lambda p: collect_and_send(1, 0, p))
    for_parts(lambda p: collect_and_send(0, 1, p))
    for_parts(lambda p: relay(2, 0, p))
    for_parts(lambda p: relay(1, 1, p))
    for_parts(lambda p: collect(2, 0, p))
    for_parts(lambda p: collect_and_send(1, 1, p))
    for_parts(lambda p: relay(2, 1, p))
    for_parts(lambda p: collect(2, 1, p))

    def deliver(p):
        for c in range(2):
            for half in range(2):
                out_ref[p, c, half] = block(2, c, p, half, coord(me, (p + 2) % 3))[...]

    for_parts(deliver)

    meta_copy.wait_send()

    @pl.loop(0, LOADS)
    def _(m):
        pair_copy(m).wait_send()

    for ph in range(3):
        for c in range(2):
            @pl.loop(0, 3)
            def _(p):
                for kind in range(3):
                    for half in range(2):
                        copy(ph, c, p, kind, half).wait_send()


def gain_kernel(sums_ref, cut_ref, feat_ref, thr_ref, reg_ref, gain_ref, leaf_ref, value_ref):
    reg = reg_ref[0]
    sums = sums_ref[...].reshape(192, 128)
    lane = lax.broadcasted_iota(jnp.int32, (128, 256), 0)
    col = lax.broadcasted_iota(jnp.int32, (128, 256), 1)
    same = (lane // 64 == col // 64 % 2) & (lane // 32 % 2 == col // 128)
    under = lane % 32 + 32
    hit = under == col % 64 + 1
    for _ in range(5):
        under = under // 2
        hit = hit | (under == col % 64 + 1)
    pick = jnp.where(same & hit, 1.0, 0.0).astype(BF16)
    hi = sums.astype(BF16)
    rest = sums - hi.astype(F32)
    mid = rest.astype(BF16)
    low = (rest - mid.astype(F32)).astype(BF16)
    nodes = jnp.dot(low, pick, preferred_element_type=F32) + jnp.dot(mid, pick, preferred_element_type=F32) + jnp.dot(hi, pick, preferred_element_type=F32)
    grad = nodes[:, :128].reshape(3, 8, 8, 128)
    hess = nodes[:, 128:].reshape(3, 8, 8, 128)
    upper = lax.broadcasted_iota(jnp.int32, (8, 128), 1) >= 64

    def score(g, h):
        return g * g / (h + reg)

    for p in range(3):
        g_all, h_all = grad[p, 7], hess[p, 7]
        g_all = jnp.where(upper, g_all, pltpu.roll(g_all, 64, 1))
        h_all = jnp.where(upper, h_all, pltpu.roll(h_all, 64, 1))
        whole = score(g_all, h_all)
        for q in range(8):
            g_left, h_left = grad[p, q], hess[p, q]
            gain = 0.5 * (score(g_left, h_left) + score(g_all - g_left, h_all - h_left) - whole)
            gain_ref[2 * q, pl.ds(8 * p, 8), :] = gain[:, :63]
            if q < 7:
                gain_ref[2 * q + 1, pl.ds(8 * p, 8), :] = pltpu.roll(gain, 64, 1)[:, :63]
    last = sums_ref[0, 1, 1, 1]
    g_leaf, h_leaf = pltpu.roll(last, 64, 1), pltpu.roll(last, 32, 1)
    leaf_ref[...] = (-g_leaf / (h_leaf + reg))[0:1, :LEAVES]
    lanes = lax.broadcasted_iota(jnp.int32, (1, 128), 1)
    steps = lax.broadcasted_iota(jnp.int32, (BINS - 1, 128), 0)
    value = jnp.zeros((1, 128), F32)
    for j in range(INNER):
        feat = feat_ref[j]
        tile = cut_ref[:, pl.ds(pl.multiple_of(feat // 128 * 128, 128), 128)]
        one = jnp.sum(jnp.where(steps == thr_ref[j], tile, 0.0), axis=0, keepdims=True)
        one = jnp.sum(jnp.where(lanes == feat % 128, one, 0.0), axis=1, keepdims=True)
        value = jnp.where(lanes == j, one, value)
    value_ref[...] = value[:, :INNER]


def solution(mesh):
    row_spec = P(('trees', 'data'))
    vmem = pl.BlockSpec(memory_space=pltpu.VMEM)
    smem = pl.BlockSpec(memory_space=pltpu.SMEM)
    hbm = pl.BlockSpec(memory_space=pl.ANY)

    def device_fn(bin_codes, gradient, hessian, valid_rows, split_feat, split_thr, cut_values, reg_lambda):
        sums = pl.pallas_call(
            hist_kernel,
            out_shape=jax.ShapeDtypeStruct((3, 2, 2, 2, 8, 128), F32),
            in_specs=[hbm, vmem, vmem, smem, smem, smem],
            out_specs=vmem,
            scratch_shapes=[
                pltpu.VMEM((LOADS, ROWS, SLAB), jnp.int32),
                pltpu.VMEM((64, 2, 24, ROWS), F32),
                pltpu.VMEM((64, 24, ROWS), F32),
                pltpu.VMEM((3, 4, 4, 4, 16, 2 * ROWS), BF16),
                pltpu.VMEM((2, 8, ROWS), F32),
                pltpu.VMEM((2 * ROWS, 256), BF16),
                pltpu.VMEM((3, 2, 4, 2, 4, 8, 8, 128), F32),
                pltpu.VMEM((3, 2, 3, 2, 4, 8, 8, 128), F32),
                pltpu.VMEM((3, 2, 3, 2, 8, 8, 128), F32),
                pltpu.VMEM((3, 2, 3, 2, 2, 8, 128), F32),
                pltpu.SemaphoreType.DMA((LOADS,)),
                pltpu.SemaphoreType.DMA((LOADS + 1,)),
                pltpu.SemaphoreType.DMA((LOADS + 1,)),
                pltpu.SemaphoreType.DMA((108,)),
                pltpu.SemaphoreType.DMA((108,)),
            ],
            compiler_params=pltpu.CompilerParams(collective_id=0, has_side_effects=True, vmem_limit_bytes=60 * 1024 * 1024),
            name='hist',
        )(bin_codes, gradient.reshape(1, ROWS), hessian.reshape(1, ROWS), valid_rows, split_feat, split_thr)
        gain, leaf, value = pl.pallas_call(
            gain_kernel,
            out_shape=(jax.ShapeDtypeStruct((BINS - 1, FEATS // 128, 63), F32), jax.ShapeDtypeStruct((1, LEAVES), F32), jax.ShapeDtypeStruct((1, INNER), F32)),
            in_specs=[vmem, vmem, smem, smem, smem],
            out_specs=(vmem, vmem, vmem),
            name='gain',
        )(sums, cut_values.T, split_feat, split_thr, reg_lambda)
        return jnp.transpose(gain, (2, 1, 0)), leaf.reshape(LEAVES), value.reshape(INNER)

    return jax.shard_map(device_fn, mesh=mesh, in_specs=(P(('trees', 'data'), None), row_spec, row_spec, row_spec, P('trees'), P('trees'), P('trees', None), P('trees')), out_specs=(P(None, ('trees', 'data'), None), P('trees'), P('trees')), check_vma=False)
```

```python
import functools
import jax
import jax.numpy as jnp
from jax import lax
from jax.experimental import pallas as pl
from jax.experimental.pallas import tpu as pltpu
from jax.sharding import PartitionSpec as P

F32 = jnp.float32
BF16 = jnp.bfloat16
ROWS = 512
FEATS = 3072
BINS = 16
LEAVES = 32
INNER = 31
LOADS = 8
SLAB = FEATS // LOADS


def pow4(dim):
    return 1 + 3 * dim * (3 * dim - 1) // 2


def coord(me, dim):
    return (me // 2) // pow4(dim) % 4


def neighbour(me, dim, step):
    at = coord(me, dim)
    return me + ((at + step + 4) % 4 - at) * 2 * pow4(dim)


def hist_kernel(codes_hbm, grad_ref, hess_ref, valid_ref, feat_ref, thr_ref, cut_hbm, out_ref, value_ref,
                raw, turned, turned_rx, codes2, meta, weights, cuts, hist, rx1, rx2, rx3,
                load_sem, pair_send, pair_recv, send_sem, recv_sem):
    me = lax.axis_index('data')
    core = me % 2
    partner = me + 1 - 2 * core

    def remote(src, dst, s_sem, r_sem, device):
        return pltpu.make_async_remote_copy(src_ref=src, dst_ref=dst, send_sem=s_sem, recv_sem=r_sem, device_id=(0, device), device_id_type=pl.DeviceIdType.MESH)

    def load(m):
        return pltpu.make_async_copy(codes_hbm.at[:, pl.ds(m * SLAB, SLAB)], raw.at[m], load_sem.at[m])

    for m in range(LOADS):
        load(m).start()
    barrier = pltpu.get_barrier_semaphore()
    pl.semaphore_signal(barrier, inc=1, device_id=(0, partner), device_id_type=pl.DeviceIdType.MESH)
    for dim in range(3):
        for step in (1, 2, 3):
            pl.semaphore_signal(barrier, inc=1, device_id=(0, neighbour(me, dim, step)), device_id_type=pl.DeviceIdType.MESH)
    pl.semaphore_wait(barrier, 10)

    def pair_copy(m):
        return remote(turned.at[pl.ds(m * 8, 8), 1 - core], turned_rx.at[pl.ds(m * 8, 8)], pair_send.at[0], pair_recv.at[m], partner)

    meta_copy = remote(meta.at[0], meta.at[1], pair_send.at[1], pair_recv.at[LOADS], partner)

    def fill_codes(source, lane0, chip):
        where = (chip % 4, chip // 4 % 4, chip // 16)
        for p in range(3):
            v = source(p)
            codes2[p, where[p], where[(p + 1) % 3], where[(p + 2) % 3], :, pl.ds(lane0, ROWS)] = jnp.concatenate([v, v - 1.0], axis=0).astype(BF16)

    def fill_own(m):
        for k in range(8):
            chip = m * 8 + k
            fill_codes(lambda p: turned[chip, core, pl.ds(8 * p, 8), :], 0, chip)

    def turn(m):
        block = raw[m].astype(F32).astype(BF16)
        turned[pl.ds(m * 8, 8)] = block.T.astype(F32).reshape(8, 2, 24, ROWS)

    load(0).wait()
    turn(0)
    pair_copy(0).start()

    @pl.loop(1, LOADS)
    def _(m):
        load(m).wait()
        fill_own(m - 1)
        turn(m)
        pair_copy(m).start()

    @pl.loop(0, FEATS // 128)
    def _(k):
        pltpu.make_async_copy(cut_hbm.at[:, pl.ds(k * 128, 128)], cuts.at[k], load_sem.at[LOADS]).start()

    fill_own(LOADS - 1)

    def goes_right(j):
        feat = feat_ref[j]
        column = turned[feat // 48, feat // 24 % 2, pl.ds(feat % 24, 1), :]
        return (column > thr_ref[j].astype(F32)).astype(jnp.int32)

    leaf = goes_right(0)
    for level in range(1, 5):
        width = 2 ** level
        bit = goes_right(width - 1)
        for n in range(1, width):
            bit = jnp.where(leaf == n, goes_right(width - 1 + n), bit)
        leaf = 2 * leaf + bit
    live = lax.broadcasted_iota(jnp.int32, (1, ROWS), 1) < valid_ref[0]
    grad = jnp.where(live, grad_ref[...], 0.0)
    hess = jnp.where(live, hess_ref[...], 0.0)
    meta[0] = jnp.concatenate([grad, hess, leaf.astype(F32), jnp.zeros((5, ROWS), F32)], axis=0)
    meta_copy.start()

    def split3(v):
        hi = v.astype(BF16).astype(F32)
        mid = (v - hi).astype(BF16).astype(F32)
        return hi, mid, v - hi - mid

    def fill_weights(side):
        for k in range(ROWS // 128):
            lanes = pl.ds(k * 128, 128)
            g3 = split3(meta[side, 0:1, lanes])
            h3 = split3(meta[side, 1:2, lanes])
            hit = meta[side, 2:3, lanes] == lax.broadcasted_iota(jnp.int32, (LEAVES, 128), 0).astype(F32)
            rows = []
            for i in range(3):
                rows.append(jnp.where(hit, g3[i], 0.0))
                rows.append(jnp.where(hit, h3[i], 0.0))
            rows.append(jnp.zeros((64, 128), F32))
            weights[pl.ds(side * ROWS + k * 128, 128), :] = jnp.concatenate(rows, axis=0).T.astype(BF16)

    fill_weights(0)

    def block(ph, c, p, half, j):
        if ph == 0:
            return hist.at[p, c, j, half]
        return hist.at[p, c, coord(me, p), half, j]

    landings = (rx1, rx2)

    def copy(ph, c, p, kind, half):
        dim = (p + ph) % 3
        at = coord(me, dim)
        step = 1 if (kind == 1) == (half == 1) else -1
        j = (at + 2) % 4 if kind == 0 else (at + step + 4) % 4
        s = ((ph * 2 + c) * 3 + p) * 2 + (0 if kind == 0 else 1)
        return remote(block(ph, c, p, half, j), landings[ph].at[p, c, kind, half], send_sem.at[ph], recv_sem.at[s], neighbour(me, dim, step))

    def wait_landed(ph, c, p, kind, count):
        s = ((ph * 2 + c) * 3 + p) * 2 + (0 if kind == 0 else 1)
        place = landings[ph].at[p, c, pl.ds(kind, count)]
        remote(place, place, send_sem.at[ph], recv_sem.at[s], partner).wait_recv()

    def send_far(ph, c, p):
        copy(ph, c, p, 0, 0).start()
        copy(ph, c, p, 0, 1).start()

    def send_near(ph, c, p):
        copy(ph, c, p, 1, 1).start()
        copy(ph, c, p, 1, 0).start()

    def relay(ph, c, p):
        at = coord(me, (p + ph) % 3)
        wait_landed(ph, c, p, 0, 1)
        for half in range(2):
            mine = block(ph, c, p, half, (at + (1, 3)[half]) % 4)
            mine[...] = mine[...] + landings[ph][p, c, 0, half]
            copy(ph, c, p, 2, half).start()

    def collect(ph, c, p):
        at = coord(me, (p + ph) % 3)
        wait_landed(ph, c, p, 1, 2)
        for half in range(2):
            mine = block(ph, c, p, half, at)
            total = mine[...] + landings[ph][p, c, 1, half] + landings[ph][p, c, 2, half]
            mine[...] = total
        if ph == 0:
            send_far(1, c, p)
            send_near(1, c, p)
        else:
            for step in (2, 1, 3):
                last_copy(c, p, step).start()

    def last_block(c, p, j):
        return hist.at[p, c, coord(me, p), :, coord(me, (p + 1) % 3), pl.ds(2 * j, 2)]

    def last_copy(c, p, step):
        dim = (p + 2) % 3
        j = (coord(me, dim) + step) % 4
        return remote(last_block(c, p, j), rx3.at[p, c, step - 1], send_sem.at[2], recv_sem.at[24 + 3 * c + p], neighbour(me, dim, step))

    def last_collect(c, p):
        remote(rx3.at[p, c], rx3.at[p, c], send_sem.at[2], recv_sem.at[24 + 3 * c + p], partner).wait_recv()
        out_ref[p, c] = last_block(c, p, coord(me, (p + 2) % 3))[...] + rx3[p, c, 0] + rx3[p, c, 1] + rx3[p, c, 2]

    first_half = lax.broadcasted_iota(jnp.int32, (64, 8, 128), 2) < 64

    def unit(c, p, jj, lane0, lanes, add):
        ahead = (2 + 3 * jj + (jj // 2) * (7 - 2 * jj)) % 4
        ja = (coord(me, p) + ahead) % 4
        bounds = [jnp.full((16, lanes), (8 * c + 2 * k).astype(F32), F32).astype(BF16) for k in range(4)]
        one = jnp.asarray(1, BF16)
        zero = jnp.asarray(0, BF16)
        pieces = []
        for half in range(2):
            for jb in range(4):
                for jc in range(4):
                    code = codes2[p, ja, jb, jc, :, pl.ds(lane0, lanes)]
                    for q in range(2):
                        pieces.append(jnp.where(code <= bounds[half * 2 + q], one, zero))
        left = jnp.concatenate(pieces, axis=0)
        sums = jnp.dot(left, weights[pl.ds(lane0, lanes), :], preferred_element_type=F32)
        sums = (sums[:, :128] + sums[:, 128:]).reshape(64, 2, 8, 128)
        even, odd = sums[:, 0], sums[:, 1]
        keep = jnp.where(first_half, even, odd)
        turn = jnp.where(first_half, odd, even).reshape(512, 128)
        both = (keep + pltpu.roll(turn, 64, 1).reshape(64, 8, 128)).reshape(2, 4, 8, 8, 128)
        if add:
            both = both + hist[p, c, ja]
        hist[p, c, ja] = both

    zero_c = jnp.int32(0)

    @pl.loop(0, 2)
    def _(jj):
        for p in range(3):
            unit(zero_c, p, jj, 0, ROWS, False)

    @pl.loop(0, LOADS)
    def _(m):
        pair_copy(m).wait_recv()
        for k in range(8):
            chip = m * 8 + k
            fill_codes(lambda p: turned_rx[chip, pl.ds(8 * p, 8), :], ROWS, chip)

    meta_copy.wait_recv()
    fill_weights(1)

    def for_parts(task, *args):
        for p in range(3):
            task(*args, p)

    @pl.loop(0, 2)
    def _(jj):
        for p in range(3):
            unit(zero_c, p, jj, ROWS, ROWS, True)

        @pl.when(jj == 0)
        def _():
            for_parts(send_far, 0, 0)

        @pl.when(jj == 1)
        def _():
            for p in range(3):
                copy(0, 0, p, 1, 1).start()

    @pl.loop(2, 8)
    def _(b):
        c, jj = b // 4, b % 4
        for p in range(3):
            unit(c, p, jj, 0, 2 * ROWS, False)

        @pl.when(jj == 0)
        def _():
            for_parts(send_far, 0, c)

        @pl.when(jj == 1)
        def _():
            for p in range(3):
                copy(0, c, p, 1, 1).start()

        @pl.when(jj == 2)
        def _():
            for p in range(3):
                copy(0, c, p, 1, 0).start()

        @pl.when(b == 3)
        def _():
            for_parts(relay, 0, 0)

        @pl.when(b == 6)
        def _():
            for_parts(collect, 0, 0)

    for_parts(relay, 0, 1)

    pltpu.make_async_copy(cuts, cuts, load_sem.at[LOADS]).wait()
    lanes = lax.broadcasted_iota(jnp.int32, (1, 128), 1)
    steps = lax.broadcasted_iota(jnp.int32, (BINS - 1, 128), 0)
    value = jnp.zeros((1, 128), F32)
    for j in range(INNER):
        feat = feat_ref[j]
        one = jnp.sum(jnp.where(steps == thr_ref[j], cuts[feat // 128], 0.0), axis=0, keepdims=True)
        one = jnp.sum(jnp.where(lanes == feat % 128, one, 0.0), axis=1, keepdims=True)
        value = jnp.where(lanes == j, one, value)
    value_ref[...] = value

    for_parts(relay, 1, 0)
    for_parts(collect, 0, 1)
    for_parts(collect, 1, 0)
    for_parts(relay, 1, 1)
    for_parts(last_collect, 0)
    for_parts(collect, 1, 1)
    for_parts(last_collect, 1)

    meta_copy.wait_send()
    remote(turned_rx, turned_rx, pair_send.at[0], pair_recv.at[0], partner).wait_send()
    for ph, place in enumerate((rx1, rx2, rx3)):
        remote(place, place, send_sem.at[ph], recv_sem.at[0], partner).wait_send()


def gain_kernel(sums_ref, found_ref, reg_ref, gain_ref, leaf_ref, value_ref):
    reg = reg_ref[0]
    sums = sums_ref[...].reshape(192, 128)
    lane = lax.broadcasted_iota(jnp.int32, (128, 256), 0)
    col = lax.broadcasted_iota(jnp.int32, (128, 256), 1)
    same = (lane // 64 == col // 64 % 2) & (lane // 32 % 2 == col // 128)
    under = lane % 32 + 32
    hit = under == col % 64 + 1
    for _ in range(5):
        under = under // 2
        hit = hit | (under == col % 64 + 1)
    pick = jnp.where(same & hit, 1.0, 0.0).astype(BF16)
    hi = sums.astype(BF16)
    rest = sums - hi.astype(F32)
    mid = rest.astype(BF16)
    low = (rest - mid.astype(F32)).astype(BF16)
    nodes = jnp.dot(low, pick, preferred_element_type=F32) + jnp.dot(mid, pick, preferred_element_type=F32) + jnp.dot(hi, pick, preferred_element_type=F32)
    grad = nodes[:, :128].reshape(3, 8, 8, 128)
    hess = nodes[:, 128:].reshape(3, 8, 8, 128)
    upper = lax.broadcasted_iota(jnp.int32, (8, 128), 1) >= 64

    def score(g, h):
        return g * g / (h + reg)

    for p in range(3):
        g_all, h_all = grad[p, 7], hess[p, 7]
        g_all = jnp.where(upper, g_all, pltpu.roll(g_all, 64, 1))
        h_all = jnp.where(upper, h_all, pltpu.roll(h_all, 64, 1))
        whole = score(g_all, h_all)
        for q in range(8):
            g_left, h_left = grad[p, q], hess[p, q]
            gain = 0.5 * (score(g_left, h_left) + score(g_all - g_left, h_all - h_left) - whole)
            gain_ref[2 * q, pl.ds(8 * p, 8), :] = gain[:, :63]
            if q < 7:
                gain_ref[2 * q + 1, pl.ds(8 * p, 8), :] = pltpu.roll(gain, 64, 1)[:, :63]
    last = sums_ref[0, 1, 1, 1]
    g_leaf, h_leaf = pltpu.roll(last, 64, 1), pltpu.roll(last, 32, 1)
    leaf_ref[...] = (-g_leaf / (h_leaf + reg))[0:1, :LEAVES]
    value_ref[...] = found_ref[:, :INNER]


def solution(mesh):
    row_spec = P(('trees', 'data'))
    vmem = pl.BlockSpec(memory_space=pltpu.VMEM)
    smem = pl.BlockSpec(memory_space=pltpu.SMEM)
    hbm = pl.BlockSpec(memory_space=pl.ANY)

    def device_fn(bin_codes, gradient, hessian, valid_rows, split_feat, split_thr, cut_values, reg_lambda):
        sums, found = pl.pallas_call(
            hist_kernel,
            out_shape=(jax.ShapeDtypeStruct((3, 2, 2, 2, 8, 128), F32), jax.ShapeDtypeStruct((1, 128), F32)),
            in_specs=[hbm, vmem, vmem, smem, smem, smem, hbm],
            out_specs=(vmem, vmem),
            scratch_shapes=[
                pltpu.VMEM((LOADS, ROWS, SLAB), jnp.int32),
                pltpu.VMEM((64, 2, 24, ROWS), F32),
                pltpu.VMEM((64, 24, ROWS), F32),
                pltpu.VMEM((3, 4, 4, 4, 16, 2 * ROWS), BF16),
                pltpu.VMEM((2, 8, ROWS), F32),
                pltpu.VMEM((2 * ROWS, 256), BF16),
                pltpu.VMEM((FEATS // 128, BINS - 1, 128), F32),
                pltpu.VMEM((3, 2, 4, 2, 4, 8, 8, 128), F32),
                pltpu.VMEM((3, 2, 3, 2, 4, 8, 8, 128), F32),
                pltpu.VMEM((3, 2, 3, 2, 8, 8, 128), F32),
                pltpu.VMEM((3, 2, 3, 2, 2, 8, 128), F32),
                pltpu.SemaphoreType.DMA((LOADS + 1,)),
                pltpu.SemaphoreType.DMA((2,)),
                pltpu.SemaphoreType.DMA((LOADS + 1,)),
                pltpu.SemaphoreType.DMA((3,)),
                pltpu.SemaphoreType.DMA((30,)),
            ],
            compiler_params=pltpu.CompilerParams(collective_id=0, has_side_effects=True, vmem_limit_bytes=60 * 1024 * 1024),
            name='hist',
        )(bin_codes, gradient.reshape(1, ROWS), hessian.reshape(1, ROWS), valid_rows, split_feat, split_thr, cut_values.T)
        gain, leaf, value = pl.pallas_call(
            gain_kernel,
            out_shape=(jax.ShapeDtypeStruct((BINS - 1, FEATS // 128, 63), F32), jax.ShapeDtypeStruct((1, LEAVES), F32), jax.ShapeDtypeStruct((1, INNER), F32)),
            in_specs=[vmem, vmem, smem],
            out_specs=(vmem, vmem, vmem),
            compiler_params=pltpu.CompilerParams(vmem_limit_bytes=4 * 1024 * 1024),
            name='gain',
        )(sums, found, reg_lambda)
        return jnp.transpose(gain, (2, 1, 0)), leaf.reshape(LEAVES), value.reshape(INNER)

    return jax.shard_map(device_fn, mesh=mesh, in_specs=(P(('trees', 'data'), None), row_spec, row_spec, row_spec, P('trees'), P('trees'), P('trees', None), P('trees')), out_specs=(P(None, ('trees', 'data'), None), P('trees'), P('trees')), check_vma=False)
```

```python
import functools
import jax
import jax.numpy as jnp
from jax import lax
from jax.experimental import pallas as pl
from jax.experimental.pallas import tpu as pltpu
from jax.sharding import PartitionSpec as P

F32 = jnp.float32
BF16 = jnp.bfloat16
ROWS = 512
FEATS = 3072
BINS = 16
LEAVES = 32
INNER = 31
LOADS = 8
SLAB = FEATS // LOADS


def pow4(dim):
    return 1 + 3 * dim * (3 * dim - 1) // 2


def coord(me, dim):
    return (me // 2) // pow4(dim) % 4


def neighbour(me, dim, step):
    at = coord(me, dim)
    return me + ((at + step + 4) % 4 - at) * 2 * pow4(dim)


def hist_kernel(codes_hbm, grad_hbm, hess_hbm, valid_hbm, feat_hbm, thr_hbm, cut_hbm, reg_hbm, out_ref, value_ref,
                grad_ref, hess_ref, valid_ref, feat_ref, thr_ref, reg_ref, raw, turned, turned_rx, codes2, meta, weights, cuts, hist, rx1, rx2, rx3,
                load_sem, pair_send, pair_recv, send_sem, recv_sem):
    me = lax.axis_index('data')
    core = me % 2
    partner = me + 1 - 2 * core

    def remote(src, dst, s_sem, r_sem, device):
        return pltpu.make_async_remote_copy(src_ref=src, dst_ref=dst, send_sem=s_sem, recv_sem=r_sem, device_id=(0, device), device_id_type=pl.DeviceIdType.MESH)

    def load(m):
        return pltpu.make_async_copy(codes_hbm.at[:, pl.ds(m * SLAB, SLAB)], raw.at[m], load_sem.at[m])

    for m in range(LOADS):
        load(m).start()
    small = [pltpu.make_async_copy(src, dst, load_sem.at[LOADS + 1 + k]) for k, (src, dst) in enumerate(
        ((grad_hbm, grad_ref), (hess_hbm, hess_ref), (valid_hbm, valid_ref), (feat_hbm, feat_ref), (thr_hbm, thr_ref), (reg_hbm, reg_ref)))]
    for one in small:
        one.start()
    barrier = pltpu.get_barrier_semaphore()
    pl.semaphore_signal(barrier, inc=1, device_id=(0, partner), device_id_type=pl.DeviceIdType.MESH)
    for dim in range(3):
        for step in (1, 2, 3):
            pl.semaphore_signal(barrier, inc=1, device_id=(0, neighbour(me, dim, step)), device_id_type=pl.DeviceIdType.MESH)
    pl.semaphore_wait(barrier, 10)

    def ahead(jj):
        return (2 + 3 * jj + (jj // 2) * (7 - 2 * jj)) % 4

    def pair_copy(jj, p):
        ja = (coord(me, p) + ahead(jj)) % 4
        other = 1 - core
        rows = pl.ds(8 * p, 8)
        if p == 0:
            src, dst = turned.at[:, :, ja, other, rows], turned_rx.at[:, :, ja, rows]
        elif p == 1:
            src, dst = turned.at[:, ja, :, other, rows], turned_rx.at[:, ja, :, rows]
        else:
            src, dst = turned.at[ja, :, :, other, rows], turned_rx.at[ja, :, :, rows]
        return remote(src, dst, pair_send.at[0], pair_recv.at[jj], partner)

    meta_copy = remote(meta.at[0], meta.at[1], pair_send.at[1], pair_recv.at[4], partner)

    def put_code(p, ja, jb, jc, lane0, v):
        codes2[p, ja, jb, jc, :, pl.ds(lane0, ROWS)] = jnp.concatenate([v, v - 1.0], axis=0).astype(BF16)

    def fill_own(m):
        z = m // 2
        for k in range(8):
            y, x = m % 2 * 2 + k // 4, k % 4
            for p in range(3):
                at = ((x, y, z), (y, z, x), (z, x, y))[p]
                put_code(p, *at, 0, turned[z, y, x, core, pl.ds(8 * p, 8), :])

    def fill_other(jj):
        for p in range(3):
            ja = (coord(me, p) + ahead(jj)) % 4
            for jb in range(4):
                for jc in range(4):
                    z, y, x = ((jc, jb, ja), (jb, ja, jc), (ja, jc, jb))[p]
                    put_code(p, ja, jb, jc, ROWS, turned_rx[z, y, x, pl.ds(8 * p, 8), :])

    def other_codes(jj):
        remote(turned_rx.at[0], turned_rx.at[0], pair_send.at[0], pair_recv.at[jj], partner).wait_recv()
        fill_other(jj)

    def turn(m):
        block = raw[m].astype(F32).astype(BF16)
        turned[m // 2, pl.ds(m % 2 * 2, 2)] = block.T.astype(F32).reshape(2, 4, 2, 24, ROWS)

    load(0).wait()
    turn(0)

    @pl.loop(1, LOADS)
    def _(m):
        load(m).wait()
        fill_own(m - 1)
        turn(m)

    for p in range(3):
        pair_copy(0, p).start()

    @pl.loop(0, FEATS // 128)
    def _(k):
        pltpu.make_async_copy(cut_hbm.at[:, pl.ds(k * 128, 128)], cuts.at[k], load_sem.at[LOADS]).start()

    fill_own(LOADS - 1)

    for one in small:
        one.wait()

    def goes_right(j):
        feat = feat_ref[j]
        column = turned[feat // 768, feat // 192 % 4, feat // 48 % 4, feat // 24 % 2, pl.ds(feat % 24, 1), :]
        return (column > thr_ref[j].astype(F32)).astype(jnp.int32)

    leaf = goes_right(0)
    for level in range(1, 5):
        width = 2 ** level
        bit = goes_right(width - 1)
        for n in range(1, width):
            bit = jnp.where(leaf == n, goes_right(width - 1 + n), bit)
        leaf = 2 * leaf + bit
    live = lax.broadcasted_iota(jnp.int32, (1, ROWS), 1) < valid_ref[...]
    grad = jnp.where(live, grad_ref[...], 0.0)
    hess = jnp.where(live, hess_ref[...], 0.0)
    meta[0] = jnp.concatenate([grad, hess, leaf.astype(F32), jnp.zeros((5, ROWS), F32)], axis=0)
    meta_copy.start()
    for jj in range(1, 4):
        for p in range(3):
            pair_copy(jj, p).start()

    def split3(v):
        hi = v.astype(BF16).astype(F32)
        mid = (v - hi).astype(BF16).astype(F32)
        return hi, mid, v - hi - mid

    def fill_weights(side):
        for k in range(ROWS // 128):
            lanes = pl.ds(k * 128, 128)
            g3 = split3(meta[side, 0:1, lanes])
            h3 = split3(meta[side, 1:2, lanes])
            hit = meta[side, 2:3, lanes] == lax.broadcasted_iota(jnp.int32, (LEAVES, 128), 0).astype(F32)
            rows = []
            for i in range(3):
                rows.append(jnp.where(hit, g3[i], 0.0))
                rows.append(jnp.where(hit, h3[i], 0.0))
            rows.append(jnp.zeros((64, 128), F32))
            weights[pl.ds(side * ROWS + k * 128, 128), :] = jnp.concatenate(rows, axis=0).T.astype(BF16)

    fill_weights(0)

    def block(ph, c, p, half, j):
        if ph == 0:
            return hist.at[p, c, j, half]
        return hist.at[p, c, coord(me, p), half, j]

    landings = (rx1, rx2)

    def copy(ph, c, p, kind, half):
        dim = (p + ph) % 3
        at = coord(me, dim)
        step = 1 if (kind == 1) == (half == 1) else -1
        j = (at + 2) % 4 if kind == 0 else (at + step + 4) % 4
        s = ((ph * 2 + c) * 3 + p) * 2 + (0 if kind == 0 else 1)
        return remote(block(ph, c, p, half, j), landings[ph].at[p, c, kind, half], send_sem.at[ph], recv_sem.at[s], neighbour(me, dim, step))

    def wait_landed(ph, c, p, kind, count):
        s = ((ph * 2 + c) * 3 + p) * 2 + (0 if kind == 0 else 1)
        place = landings[ph].at[p, c, pl.ds(kind, count)]
        remote(place, place, send_sem.at[ph], recv_sem.at[s], partner).wait_recv()

    def send_far(ph, c, p):
        copy(ph, c, p, 0, 0).start()
        copy(ph, c, p, 0, 1).start()

    def send_near(ph, c, p):
        copy(ph, c, p, 1, 1).start()
        copy(ph, c, p, 1, 0).start()

    def relay(ph, c, p):
        at = coord(me, (p + ph) % 3)
        wait_landed(ph, c, p, 0, 1)
        for half in range(2):
            mine = block(ph, c, p, half, (at + (1, 3)[half]) % 4)
            mine[...] = mine[...] + landings[ph][p, c, 0, half]
            copy(ph, c, p, 2, half).start()

    def collect(ph, c, p):
        at = coord(me, (p + ph) % 3)
        wait_landed(ph, c, p, 1, 2)
        for half in range(2):
            mine = block(ph, c, p, half, at)
            total = mine[...] + landings[ph][p, c, 1, half] + landings[ph][p, c, 2, half]
            mine[...] = total
        if ph == 0:
            send_far(1, c, p)
            send_near(1, c, p)
        else:
            for step in (2, 1, 3):
                last_copy(c, p, step).start()

    def last_block(c, p, j):
        return hist.at[p, c, coord(me, p), :, coord(me, (p + 1) % 3), pl.ds(2 * j, 2)]

    def last_copy(c, p, step):
        dim = (p + 2) % 3
        j = (coord(me, dim) + step) % 4
        return remote(last_block(c, p, j), rx3.at[p, c, step - 1], send_sem.at[2], recv_sem.at[24 + 3 * c + p], neighbour(me, dim, step))

    def last_collect(c, p):
        remote(rx3.at[p, c], rx3.at[p, c], send_sem.at[2], recv_sem.at[24 + 3 * c + p], partner).wait_recv()
        out_ref[p, c] = last_block(c, p, coord(me, (p + 2) % 3))[...] + rx3[p, c, 0] + rx3[p, c, 1] + rx3[p, c, 2]

    first_half = lax.broadcasted_iota(jnp.int32, (64, 8, 128), 2) < 64

    def unit(c, p, jj, lane0, lanes, add):
        ja = (coord(me, p) + ahead(jj)) % 4
        bounds = [jnp.full((16, lanes), (8 * c + 2 * k).astype(F32), F32).astype(BF16) for k in range(4)]
        one = jnp.asarray(1, BF16)
        zero = jnp.asarray(0, BF16)
        pieces = []
        for half in range(2):
            for jb in range(4):
                for jc in range(4):
                    code = codes2[p, ja, jb, jc, :, pl.ds(lane0, lanes)]
                    for q in range(2):
                        pieces.append(jnp.where(code <= bounds[half * 2 + q], one, zero))
        left = jnp.concatenate(pieces, axis=0)
        sums = jnp.dot(left, weights[pl.ds(lane0, lanes), :], preferred_element_type=F32)
        sums = (sums[:, :128] + sums[:, 128:]).reshape(64, 2, 8, 128)
        even, odd = sums[:, 0], sums[:, 1]
        keep = jnp.where(first_half, even, odd)
        turn = jnp.where(first_half, odd, even).reshape(512, 128)
        both = (keep + pltpu.roll(turn, 64, 1).reshape(64, 8, 128)).reshape(2, 4, 8, 8, 128)
        if add:
            both = both + hist[p, c, ja]
        hist[p, c, ja] = both

    zero = jnp.int32(0)
    for p in range(3):
        unit(zero, p, 0, 0, ROWS, False)
    other_codes(0)
    meta_copy.wait_recv()
    fill_weights(1)

    def for_parts(task, *args):
        for p in range(3):
            task(*args, p)

    for p in range(3):
        unit(zero, p, 0, ROWS, ROWS, True)
    for_parts(send_far, 0, 0)

    @pl.loop(1, 8)
    def _(b):
        c, jj = b // 4, b % 4

        @pl.when(c == 0)
        def _():
            other_codes(jj)

        for p in range(3):
            unit(c, p, jj, 0, 2 * ROWS, False)

        @pl.when(jj == 0)
        def _():
            for_parts(send_far, 0, c)

        @pl.when(jj == 1)
        def _():
            for p in range(3):
                copy(0, c, p, 1, 1).start()

        @pl.when(jj == 2)
        def _():
            for p in range(3):
                copy(0, c, p, 1, 0).start()

        @pl.when(b == 3)
        def _():
            for_parts(relay, 0, 0)

        @pl.when(b == 6)
        def _():
            for_parts(collect, 0, 0)

    for_parts(relay, 0, 1)

    pltpu.make_async_copy(cuts, cuts, load_sem.at[LOADS]).wait()
    lanes = lax.broadcasted_iota(jnp.int32, (1, 128), 1)
    steps = lax.broadcasted_iota(jnp.int32, (BINS - 1, 128), 0)
    value = jnp.zeros((1, 128), F32)
    for j in range(INNER):
        feat = feat_ref[j]
        one = jnp.sum(jnp.where(steps == thr_ref[j], cuts[feat // 128], 0.0), axis=0, keepdims=True)
        one = jnp.sum(jnp.where(lanes == feat % 128, one, 0.0), axis=1, keepdims=True)
        value = jnp.where(lanes == j, one, value)
    value_ref[...] = jnp.where(lanes == 127, reg_ref[...], value)

    for_parts(relay, 1, 0)
    for_parts(collect, 0, 1)
    for_parts(collect, 1, 0)
    for_parts(relay, 1, 1)
    for_parts(last_collect, 0)
    for_parts(collect, 1, 1)
    for_parts(last_collect, 1)

    meta_copy.wait_send()
    remote(turned_rx, turned_rx, pair_send.at[0], pair_recv.at[4], partner).wait_send()
    for ph, place in enumerate((rx1, rx2, rx3)):
        remote(place, place, send_sem.at[ph], recv_sem.at[0], partner).wait_send()


def gain_kernel(sums_ref, found_ref, gain_ref, leaf_ref, value_ref):
    reg = found_ref[0:1, 127:128]
    sums = sums_ref[...].reshape(192, 128)
    lane = lax.broadcasted_iota(jnp.int32, (128, 256), 0)
    col = lax.broadcasted_iota(jnp.int32, (128, 256), 1)
    same = (lane // 64 == col // 64 % 2) & (lane // 32 % 2 == col // 128)
    under = lane % 32 + 32
    hit = under == col % 64 + 1
    for _ in range(5):
        under = under // 2
        hit = hit | (under == col % 64 + 1)
    pick = jnp.where(same & hit, 1.0, 0.0).astype(BF16)
    hi = sums.astype(BF16)
    rest = sums - hi.astype(F32)
    mid = rest.astype(BF16)
    low = (rest - mid.astype(F32)).astype(BF16)
    nodes = jnp.dot(low, pick, preferred_element_type=F32) + jnp.dot(mid, pick, preferred_element_type=F32) + jnp.dot(hi, pick, preferred_element_type=F32)
    grad = nodes[:, :128].reshape(3, 8, 8, 128)
    hess = nodes[:, 128:].reshape(3, 8, 8, 128)
    upper = lax.broadcasted_iota(jnp.int32, (8, 128), 1) >= 64

    def score(g, h):
        return g * g / (h + reg)

    for p in range(3):
        g_all, h_all = grad[p, 7], hess[p, 7]
        g_all = jnp.where(upper, g_all, pltpu.roll(g_all, 64, 1))
        h_all = jnp.where(upper, h_all, pltpu.roll(h_all, 64, 1))
        whole = score(g_all, h_all)
        for q in range(8):
            g_left, h_left = grad[p, q], hess[p, q]
            gain = 0.5 * (score(g_left, h_left) + score(g_all - g_left, h_all - h_left) - whole)
            gain_ref[2 * q, pl.ds(8 * p, 8), :] = gain[:, :63]
            if q < 7:
                gain_ref[2 * q + 1, pl.ds(8 * p, 8), :] = pltpu.roll(gain, 64, 1)[:, :63]
    last = sums_ref[0, 1, 1, 1]
    g_leaf, h_leaf = pltpu.roll(last, 64, 1), pltpu.roll(last, 32, 1)
    leaf_ref[...] = (-g_leaf / (h_leaf + reg))[0:1, :LEAVES]
    value_ref[...] = found_ref[:, :INNER]


def solution(mesh):
    row_spec = P(('trees', 'data'))
    vmem = pl.BlockSpec(memory_space=pltpu.VMEM)
    hbm = pl.BlockSpec(memory_space=pl.ANY)

    def device_fn(bin_codes, gradient, hessian, valid_rows, split_feat, split_thr, cut_values, reg_lambda):
        sums, found = pl.pallas_call(
            hist_kernel,
            out_shape=(pltpu.VMEM((3, 2, 2, 2, 8, 128), F32), pltpu.VMEM((1, 128), F32)),
            in_specs=[hbm] * 8,
            out_specs=(vmem, vmem),
            scratch_shapes=[
                pltpu.VMEM((1, ROWS), F32),
                pltpu.VMEM((1, ROWS), F32),
                pltpu.VMEM((1, 1), jnp.int32),
                pltpu.SMEM((INNER,), jnp.int32),
                pltpu.SMEM((INNER,), jnp.int32),
                pltpu.VMEM((1, 1), F32),
                pltpu.VMEM((LOADS, ROWS, SLAB), jnp.int32),
                pltpu.VMEM((4, 4, 4, 2, 24, ROWS), F32),
                pltpu.VMEM((4, 4, 4, 24, ROWS), F32),
                pltpu.VMEM((3, 4, 4, 4, 16, 2 * ROWS), BF16),
                pltpu.VMEM((2, 8, ROWS), F32),
                pltpu.VMEM((2 * ROWS, 256), BF16),
                pltpu.VMEM((FEATS // 128, BINS - 1, 128), F32),
                pltpu.VMEM((3, 2, 4, 2, 4, 8, 8, 128), F32),
                pltpu.VMEM((3, 2, 3, 2, 4, 8, 8, 128), F32),
                pltpu.VMEM((3, 2, 3, 2, 8, 8, 128), F32),
                pltpu.VMEM((3, 2, 3, 2, 2, 8, 128), F32),
                pltpu.SemaphoreType.DMA((LOADS + 7,)),
                pltpu.SemaphoreType.DMA((2,)),
                pltpu.SemaphoreType.DMA((5,)),
                pltpu.SemaphoreType.DMA((3,)),
                pltpu.SemaphoreType.DMA((30,)),
            ],
            compiler_params=pltpu.CompilerParams(collective_id=0, has_side_effects=True, vmem_limit_bytes=60 * 1024 * 1024),
            name='hist',
        )(bin_codes, gradient.reshape(1, ROWS), hessian.reshape(1, ROWS), valid_rows.reshape(1, 1), split_feat, split_thr, cut_values.T, reg_lambda.reshape(1, 1))
        gain, leaf, value = pl.pallas_call(
            gain_kernel,
            out_shape=(jax.ShapeDtypeStruct((BINS - 1, FEATS // 128, 63), F32), jax.ShapeDtypeStruct((1, LEAVES), F32), jax.ShapeDtypeStruct((1, INNER), F32)),
            in_specs=[vmem, vmem],
            out_specs=(vmem, vmem, vmem),
            compiler_params=pltpu.CompilerParams(vmem_limit_bytes=4 * 1024 * 1024),
            name='gain',
        )(sums, found)
        return jnp.transpose(gain, (2, 1, 0)), leaf.reshape(LEAVES), value.reshape(INNER)

    return jax.shard_map(device_fn, mesh=mesh, in_specs=(P(('trees', 'data'), None), row_spec, row_spec, row_spec, P('trees'), P('trees'), P('trees', None), P('trees')), out_specs=(P(None, ('trees', 'data'), None), P('trees'), P('trees')), check_vma=False)
```

```python
import functools
import jax
import jax.numpy as jnp
from jax import lax
from jax.experimental import pallas as pl
from jax.experimental.pallas import tpu as pltpu
from jax.sharding import PartitionSpec as P

F32 = jnp.float32
BF16 = jnp.bfloat16
ROWS = 512
FEATS = 3072
BINS = 16
LEAVES = 32
INNER = 31
LOADS = 8
SLAB = FEATS // LOADS


def pow4(dim):
    return 1 + 3 * dim * (3 * dim - 1) // 2


def coord(me, dim):
    return (me // 2) // pow4(dim) % 4


def neighbour(me, dim, step):
    at = coord(me, dim)
    return me + ((at + step + 4) % 4 - at) * 2 * pow4(dim)


def hist_kernel(codes_hbm, grad_hbm, hess_hbm, valid_hbm, feat_hbm, thr_hbm, cut_hbm, reg_hbm, out_ref, value_ref,
                grad_ref, hess_ref, valid_ref, feat_ref, thr_ref, reg_ref, raw, turned, turned_rx, codes2, meta, weights, cuts, hist, rx1, rx2, rx3,
                load_sem, pair_send, pair_recv, send_sem, recv_sem):
    me = lax.axis_index('data')
    core = me % 2
    partner = me + 1 - 2 * core

    def remote(src, dst, s_sem, r_sem, device):
        return pltpu.make_async_remote_copy(src_ref=src, dst_ref=dst, send_sem=s_sem, recv_sem=r_sem, device_id=(0, device), device_id_type=pl.DeviceIdType.MESH)

    def load(m):
        return pltpu.make_async_copy(codes_hbm.at[:, pl.ds(m * SLAB, SLAB)], raw.at[m], load_sem.at[m])

    for m in range(LOADS):
        load(m).start()
    small = [pltpu.make_async_copy(src, dst, load_sem.at[LOADS + 1 + k]) for k, (src, dst) in enumerate(
        ((grad_hbm, grad_ref), (hess_hbm, hess_ref), (valid_hbm, valid_ref), (feat_hbm, feat_ref), (thr_hbm, thr_ref), (reg_hbm, reg_ref)))]
    for one in small:
        one.start()
    barrier = pltpu.get_barrier_semaphore()
    pl.semaphore_signal(barrier, inc=1, device_id=(0, partner), device_id_type=pl.DeviceIdType.MESH)
    for dim in range(3):
        for step in (1, 2, 3):
            pl.semaphore_signal(barrier, inc=1, device_id=(0, neighbour(me, dim, step)), device_id_type=pl.DeviceIdType.MESH)
    pl.semaphore_wait(barrier, 10)

    def ahead(jj):
        return (2 + 3 * jj + (jj // 2) * (7 - 2 * jj)) % 4

    def pair_copy(jj, p):
        ja = (coord(me, p) + ahead(jj)) % 4
        other = 1 - core
        rows = pl.ds(8 * p, 8)
        if p == 0:
            src, dst = turned.at[:, :, ja, other, rows], turned_rx.at[:, :, ja, rows]
        elif p == 1:
            src, dst = turned.at[:, ja, :, other, rows], turned_rx.at[:, ja, :, rows]
        else:
            src, dst = turned.at[ja, :, :, other, rows], turned_rx.at[ja, :, :, rows]
        return remote(src, dst, pair_send.at[0], pair_recv.at[jj], partner)

    meta_copy = remote(meta.at[0], meta.at[1], pair_send.at[1], pair_recv.at[4], partner)

    def put_code(p, ja, jb, jc, lane0, v):
        codes2[p, ja, jb, jc, :, pl.ds(lane0, ROWS)] = jnp.concatenate([v, v - 1.0], axis=0).astype(BF16)

    def fill_own(m):
        z = m // 2
        for k in range(8):
            y, x = m % 2 * 2 + k // 4, k % 4
            for p in range(3):
                at = ((x, y, z), (y, z, x), (z, x, y))[p]
                put_code(p, *at, 0, turned[z, y, x, core, pl.ds(8 * p, 8), :])

    def fill_other(jj):
        for p in range(3):
            ja = (coord(me, p) + ahead(jj)) % 4
            for jb in range(4):
                for jc in range(4):
                    z, y, x = ((jc, jb, ja), (jb, ja, jc), (ja, jc, jb))[p]
                    put_code(p, ja, jb, jc, ROWS, turned_rx[z, y, x, pl.ds(8 * p, 8), :])

    def other_codes(jj):
        remote(turned_rx.at[0], turned_rx.at[0], pair_send.at[0], pair_recv.at[jj], partner).wait_recv()
        fill_other(jj)

    def turn(m):
        block = raw[m].astype(F32).astype(BF16)
        turned[m // 2, pl.ds(m % 2 * 2, 2)] = block.T.astype(F32).reshape(2, 4, 2, 24, ROWS)

    load(0).wait()
    turn(0)

    @pl.loop(1, LOADS)
    def _(m):
        load(m).wait()
        fill_own(m - 1)
        turn(m)

    for p in range(3):
        pair_copy(0, p).start()

    @pl.loop(0, FEATS // 128)
    def _(k):
        pltpu.make_async_copy(cut_hbm.at[:, pl.ds(k * 128, 128)], cuts.at[k], load_sem.at[LOADS]).start()

    fill_own(LOADS - 1)

    for one in small:
        one.wait()

    def goes_right(j):
        feat = feat_ref[j]
        column = turned[feat // 768, feat // 192 % 4, feat // 48 % 4, feat // 24 % 2, pl.ds(feat % 24, 1), :]
        return (column > thr_ref[j].astype(F32)).astype(jnp.int32)

    leaf = goes_right(0)
    for level in range(1, 5):
        width = 2 ** level
        bit = goes_right(width - 1)
        for n in range(1, width):
            bit = jnp.where(leaf == n, goes_right(width - 1 + n), bit)
        leaf = 2 * leaf + bit
    live = lax.broadcasted_iota(jnp.int32, (1, ROWS), 1) < valid_ref[...]
    grad = jnp.where(live, grad_ref[...], 0.0)
    hess = jnp.where(live, hess_ref[...], 0.0)
    meta[0] = jnp.concatenate([grad, hess, leaf.astype(F32), jnp.zeros((5, ROWS), F32)], axis=0)
    meta_copy.start()
    for jj in range(1, 4):
        for p in range(3):
            pair_copy(jj, p).start()

    def split3(v):
        hi = v.astype(BF16).astype(F32)
        mid = (v - hi).astype(BF16).astype(F32)
        return hi, mid, v - hi - mid

    def fill_weights(side):
        for k in range(ROWS // 128):
            lanes = pl.ds(k * 128, 128)
            g3 = split3(meta[side, 0:1, lanes])
            h3 = split3(meta[side, 1:2, lanes])
            hit = meta[side, 2:3, lanes] == lax.broadcasted_iota(jnp.int32, (LEAVES, 128), 0).astype(F32)
            rows = []
            for i in range(3):
                rows.append(jnp.where(hit, g3[i], 0.0))
                rows.append(jnp.where(hit, h3[i], 0.0))
            rows.append(jnp.zeros((64, 128), F32))
            weights[pl.ds(side * ROWS + k * 128, 128), :] = jnp.concatenate(rows, axis=0).T.astype(BF16)

    fill_weights(0)

    def block(ph, c, p, half, j):
        if ph == 0:
            return hist.at[p, c, j, half]
        return hist.at[p, c, coord(me, p), half, j]

    landings = (rx1, rx2)

    def copy(ph, c, p, kind, half):
        dim = (p + ph) % 3
        at = coord(me, dim)
        step = 1 if (kind == 1) == (half == 1) else -1
        j = (at + 2) % 4 if kind == 0 else (at + step + 4) % 4
        s = ((ph * 2 + c) * 3 + p) * 2 + (0 if kind == 0 else 1)
        return remote(block(ph, c, p, half, j), landings[ph].at[p, c, kind, half], send_sem.at[ph], recv_sem.at[s], neighbour(me, dim, step))

    def wait_landed(ph, c, p, kind, count):
        s = ((ph * 2 + c) * 3 + p) * 2 + (0 if kind == 0 else 1)
        place = landings[ph].at[p, c, pl.ds(kind, count)]
        remote(place, place, send_sem.at[ph], recv_sem.at[s], partner).wait_recv()

    def send_far(ph, c, p):
        copy(ph, c, p, 0, 0).start()
        copy(ph, c, p, 0, 1).start()

    def send_near(ph, c, p):
        copy(ph, c, p, 1, 1).start()
        copy(ph, c, p, 1, 0).start()

    def relay(ph, c, p):
        at = coord(me, (p + ph) % 3)
        wait_landed(ph, c, p, 0, 1)
        for half in range(2):
            mine = block(ph, c, p, half, (at + (1, 3)[half]) % 4)
            mine[...] = mine[...] + landings[ph][p, c, 0, half]
            copy(ph, c, p, 2, half).start()

    def collect(ph, c, p):
        at = coord(me, (p + ph) % 3)
        wait_landed(ph, c, p, 1, 2)
        for half in range(2):
            mine = block(ph, c, p, half, at)
            total = mine[...] + landings[ph][p, c, 1, half] + landings[ph][p, c, 2, half]
            mine[...] = total
        if ph == 0:
            send_far(1, c, p)
            send_near(1, c, p)
        else:
            for step in (2, 1, 3):
                last_copy(c, p, step).start()

    def last_block(c, p, j):
        return hist.at[p, c, coord(me, p), :, coord(me, (p + 1) % 3), pl.ds(2 * j, 2)]

    def last_copy(c, p, step):
        dim = (p + 2) % 3
        j = (coord(me, dim) + step) % 4
        return remote(last_block(c, p, j), rx3.at[p, c, step - 1], send_sem.at[2], recv_sem.at[24 + 3 * c + p], neighbour(me, dim, step))

    def last_collect(c, p):
        remote(rx3.at[p, c], rx3.at[p, c], send_sem.at[2], recv_sem.at[24 + 3 * c + p], partner).wait_recv()
        out_ref[p, c] = last_block(c, p, coord(me, (p + 2) % 3))[...] + rx3[p, c, 0] + rx3[p, c, 1] + rx3[p, c, 2]

    first_half = lax.broadcasted_iota(jnp.int32, (64, 8, 128), 2) < 64

    def unit(c, p, jj, lane0, lanes, add):
        ja = (coord(me, p) + ahead(jj)) % 4
        bounds = [jnp.full((16, lanes), (8 * c + 2 * k).astype(F32), F32).astype(BF16) for k in range(4)]
        one = jnp.asarray(1, BF16)
        zero = jnp.asarray(0, BF16)
        pieces = []
        for half in range(2):
            for jb in range(4):
                for jc in range(4):
                    code = codes2[p, ja, jb, jc, :, pl.ds(lane0, lanes)]
                    for q in range(2):
                        pieces.append(jnp.where(code <= bounds[half * 2 + q], one, zero))
        left = jnp.concatenate(pieces, axis=0)
        sums = jnp.dot(left, weights[pl.ds(lane0, lanes), :], preferred_element_type=F32)
        sums = (sums[:, :128] + sums[:, 128:]).reshape(64, 2, 8, 128)
        even, odd = sums[:, 0], sums[:, 1]
        keep = jnp.where(first_half, even, odd)
        turn = jnp.where(first_half, odd, even).reshape(512, 128)
        both = (keep + pltpu.roll(turn, 64, 1).reshape(64, 8, 128)).reshape(2, 4, 8, 8, 128)
        if add:
            both = both + hist[p, c, ja]
        hist[p, c, ja] = both

    zero = jnp.int32(0)
    for p in range(3):
        unit(zero, p, 0, 0, ROWS, False)
    other_codes(0)
    meta_copy.wait_recv()
    fill_weights(1)

    def for_parts(task, *args):
        for p in range(3):
            task(*args, p)

    for p in range(3):
        unit(zero, p, 0, ROWS, ROWS, True)
    for_parts(send_far, 0, 0)

    def pick(b, *values):
        return sum((b == k + 1).astype(jnp.int32) * v for k, v in enumerate(values))

    @pl.loop(1, 8)
    def _(b):
        item = (1 - core) * pick(b, 4, 6, 1, 2, 5, 7, 3) + core * pick(b, 1, 4, 2, 5, 7, 6, 3)
        fresh = (1 - core) * pick(b, 0, 1, 1, 0, 0, 1, 0) + core * pick(b, 1, 0, 1, 0, 1, 0, 0)
        c, jj = item // 4, item % 4

        @pl.when(fresh == 1)
        def _():
            other_codes(jj)

        for p in range(3):
            unit(c, p, jj, 0, 2 * ROWS, False)

        @pl.when(jj == 0)
        def _():
            for_parts(send_far, 0, c)

        @pl.when(jj == 1)
        def _():
            for p in range(3):
                copy(0, c, p, 1, 1).start()

        @pl.when(jj == 2)
        def _():
            for p in range(3):
                copy(0, c, p, 1, 0).start()

        @pl.when((core == 0) & (b == 4))
        def _():
            for_parts(relay, 0, 0)

        @pl.when((core == 0) & (b == 5))
        def _():
            for_parts(relay, 0, 1)

    @pl.when(core == 1)
    def _():
        for_parts(relay, 0, 0)
        for_parts(relay, 0, 1)

    pltpu.make_async_copy(cuts, cuts, load_sem.at[LOADS]).wait()
    lanes = lax.broadcasted_iota(jnp.int32, (1, 128), 1)
    steps = lax.broadcasted_iota(jnp.int32, (BINS - 1, 128), 0)
    value = jnp.zeros((1, 128), F32)
    for j in range(INNER):
        feat = feat_ref[j]
        one = jnp.sum(jnp.where(steps == thr_ref[j], cuts[feat // 128], 0.0), axis=0, keepdims=True)
        one = jnp.sum(jnp.where(lanes == feat % 128, one, 0.0), axis=1, keepdims=True)
        value = jnp.where(lanes == j, one, value)
    value_ref[...] = jnp.where(lanes == 127, reg_ref[...], value)

    for_parts(collect, 0, 0)
    for_parts(collect, 0, 1)
    for_parts(relay, 1, 0)
    for_parts(relay, 1, 1)
    for_parts(collect, 1, 0)
    for_parts(collect, 1, 1)
    for_parts(last_collect, 0)
    for_parts(last_collect, 1)

    meta_copy.wait_send()
    remote(turned_rx, turned_rx, pair_send.at[0], pair_recv.at[4], partner).wait_send()
    for ph, place in enumerate((rx1, rx2, rx3)):
        remote(place, place, send_sem.at[ph], recv_sem.at[0], partner).wait_send()


def gain_kernel(sums_ref, found_ref, gain_ref, leaf_ref, value_ref):
    reg = found_ref[0:1, 127:128]
    sums = sums_ref[...].reshape(192, 128)
    lane = lax.broadcasted_iota(jnp.int32, (128, 256), 0)
    col = lax.broadcasted_iota(jnp.int32, (128, 256), 1)
    same = (lane // 64 == col // 64 % 2) & (lane // 32 % 2 == col // 128)
    under = lane % 32 + 32
    hit = under == col % 64 + 1
    for _ in range(5):
        under = under // 2
        hit = hit | (under == col % 64 + 1)
    pick = jnp.where(same & hit, 1.0, 0.0).astype(BF16)
    hi = sums.astype(BF16)
    rest = sums - hi.astype(F32)
    mid = rest.astype(BF16)
    low = (rest - mid.astype(F32)).astype(BF16)
    nodes = jnp.dot(low, pick, preferred_element_type=F32) + jnp.dot(mid, pick, preferred_element_type=F32) + jnp.dot(hi, pick, preferred_element_type=F32)
    grad = nodes[:, :128].reshape(3, 8, 8, 128)
    hess = nodes[:, 128:].reshape(3, 8, 8, 128)
    upper = lax.broadcasted_iota(jnp.int32, (8, 128), 1) >= 64

    def score(g, h):
        return g * g / (h + reg)

    for p in range(3):
        g_all, h_all = grad[p, 7], hess[p, 7]
        g_all = jnp.where(upper, g_all, pltpu.roll(g_all, 64, 1))
        h_all = jnp.where(upper, h_all, pltpu.roll(h_all, 64, 1))
        whole = score(g_all, h_all)
        for q in range(8):
            g_left, h_left = grad[p, q], hess[p, q]
            gain = 0.5 * (score(g_left, h_left) + score(g_all - g_left, h_all - h_left) - whole)
            gain_ref[2 * q, pl.ds(8 * p, 8), :] = gain[:, :63]
            if q < 7:
                gain_ref[2 * q + 1, pl.ds(8 * p, 8), :] = pltpu.roll(gain, 64, 1)[:, :63]
    last = sums_ref[0, 1, 1, 1]
    g_leaf, h_leaf = pltpu.roll(last, 64, 1), pltpu.roll(last, 32, 1)
    leaf_ref[...] = (-g_leaf / (h_leaf + reg))[0:1, :LEAVES]
    value_ref[...] = found_ref[:, :INNER]


def solution(mesh):
    row_spec = P(('trees', 'data'))
    vmem = pl.BlockSpec(memory_space=pltpu.VMEM)
    hbm = pl.BlockSpec(memory_space=pl.ANY)

    def device_fn(bin_codes, gradient, hessian, valid_rows, split_feat, split_thr, cut_values, reg_lambda):
        sums, found = pl.pallas_call(
            hist_kernel,
            out_shape=(pltpu.VMEM((3, 2, 2, 2, 8, 128), F32), pltpu.VMEM((1, 128), F32)),
            in_specs=[hbm] * 8,
            out_specs=(vmem, vmem),
            scratch_shapes=[
                pltpu.VMEM((1, ROWS), F32),
                pltpu.VMEM((1, ROWS), F32),
                pltpu.VMEM((1, 1), jnp.int32),
                pltpu.SMEM((INNER,), jnp.int32),
                pltpu.SMEM((INNER,), jnp.int32),
                pltpu.VMEM((1, 1), F32),
                pltpu.VMEM((LOADS, ROWS, SLAB), jnp.int32),
                pltpu.VMEM((4, 4, 4, 2, 24, ROWS), F32),
                pltpu.VMEM((4, 4, 4, 24, ROWS), F32),
                pltpu.VMEM((3, 4, 4, 4, 16, 2 * ROWS), BF16),
                pltpu.VMEM((2, 8, ROWS), F32),
                pltpu.VMEM((2 * ROWS, 256), BF16),
                pltpu.VMEM((FEATS // 128, BINS - 1, 128), F32),
                pltpu.VMEM((3, 2, 4, 2, 4, 8, 8, 128), F32),
                pltpu.VMEM((3, 2, 3, 2, 4, 8, 8, 128), F32),
                pltpu.VMEM((3, 2, 3, 2, 8, 8, 128), F32),
                pltpu.VMEM((3, 2, 3, 2, 2, 8, 128), F32),
                pltpu.SemaphoreType.DMA((LOADS + 7,)),
                pltpu.SemaphoreType.DMA((2,)),
                pltpu.SemaphoreType.DMA((5,)),
                pltpu.SemaphoreType.DMA((3,)),
                pltpu.SemaphoreType.DMA((30,)),
            ],
            compiler_params=pltpu.CompilerParams(collective_id=0, has_side_effects=True, vmem_limit_bytes=60 * 1024 * 1024),
            name='hist',
        )(bin_codes, gradient.reshape(1, ROWS), hessian.reshape(1, ROWS), valid_rows.reshape(1, 1), split_feat, split_thr, cut_values.T, reg_lambda.reshape(1, 1))
        gain, leaf, value = pl.pallas_call(
            gain_kernel,
            out_shape=(jax.ShapeDtypeStruct((BINS - 1, FEATS // 128, 63), F32), jax.ShapeDtypeStruct((1, LEAVES), F32), jax.ShapeDtypeStruct((1, INNER), F32)),
            in_specs=[vmem, vmem],
            out_specs=(vmem, vmem, vmem),
            compiler_params=pltpu.CompilerParams(vmem_limit_bytes=4 * 1024 * 1024),
            name='gain',
        )(sums, found)
        return jnp.transpose(gain, (2, 1, 0)), leaf.reshape(LEAVES), value.reshape(INNER)

    return jax.shard_map(device_fn, mesh=mesh, in_specs=(P(('trees', 'data'), None), row_spec, row_spec, row_spec, P('trees'), P('trees'), P('trees', None), P('trees')), out_specs=(P(None, ('trees', 'data'), None), P('trees'), P('trees')), check_vma=False)
```

```python
import functools
import jax
import jax.numpy as jnp
from jax import lax
from jax.experimental import pallas as pl
from jax.experimental.pallas import tpu as pltpu
from jax.sharding import PartitionSpec as P

F32 = jnp.float32
BF16 = jnp.bfloat16
ROWS = 512
FEATS = 3072
BINS = 16
LEAVES = 32
INNER = 31
LOADS = 8
SLAB = FEATS // LOADS
GROUP = 128


def pow4(dim):
    return 1 + 3 * dim * (3 * dim - 1) // 2


def coord(me, dim):
    return (me // 2) // pow4(dim) % 4


def neighbour(me, dim, step):
    at = coord(me, dim)
    return me + ((at + step + 4) % 4 - at) * 2 * pow4(dim)


def hist_kernel(codes_hbm, grad_hbm, hess_hbm, valid_hbm, feat_hbm, thr_hbm, cut_hbm, reg_hbm, out_ref, value_ref,
                grad_ref, hess_ref, valid_ref, feat_ref, thr_ref, reg_ref, raw, turned, turned_rx, codes2, meta, weights, cuts, hist, rx1, rx2, rx3,
                load_sem, pair_send, pair_recv, send_sem, recv_sem):
    me = lax.axis_index('data')
    core = me % 2
    partner = me + 1 - 2 * core

    def remote(src, dst, s_sem, r_sem, device):
        return pltpu.make_async_remote_copy(src_ref=src, dst_ref=dst, send_sem=s_sem, recv_sem=r_sem, device_id=(0, device), device_id_type=pl.DeviceIdType.MESH)

    def load(m):
        return pltpu.make_async_copy(codes_hbm.at[:, pl.ds(m * SLAB, SLAB)], raw.at[m], load_sem.at[m])

    for m in range(LOADS):
        load(m).start()
    small = [pltpu.make_async_copy(src, dst, load_sem.at[LOADS + 1 + k]) for k, (src, dst) in enumerate(
        ((grad_hbm, grad_ref), (hess_hbm, hess_ref), (valid_hbm, valid_ref), (feat_hbm, feat_ref), (thr_hbm, thr_ref), (reg_hbm, reg_ref)))]
    for one in small:
        one.start()
    barrier = pltpu.get_barrier_semaphore()
    pl.semaphore_signal(barrier, inc=1, device_id=(0, partner), device_id_type=pl.DeviceIdType.MESH)
    for dim in range(3):
        for step in (1, 2, 3):
            pl.semaphore_signal(barrier, inc=1, device_id=(0, neighbour(me, dim, step)), device_id_type=pl.DeviceIdType.MESH)
    pl.semaphore_wait(barrier, 10)

    def ahead(jj):
        return (2 + 3 * jj + (jj // 2) * (7 - 2 * jj)) % 4

    def pair_copy(jj, p):
        ja = (coord(me, p) + ahead(jj)) % 4
        other = 1 - core
        rows = pl.ds(8 * p, 8)
        if p == 0:
            src, dst = turned.at[:, :, ja, other, rows], turned_rx.at[:, :, ja, rows]
        elif p == 1:
            src, dst = turned.at[:, ja, :, other, rows], turned_rx.at[:, ja, :, rows]
        else:
            src, dst = turned.at[ja, :, :, other, rows], turned_rx.at[ja, :, :, rows]
        return remote(src, dst, pair_send.at[0], pair_recv.at[jj], partner)

    meta_copy = remote(meta.at[0], meta.at[1], pair_send.at[1], pair_recv.at[4], partner)

    def put_code(p, ja, jb, jc, lane0, v):
        codes2[p, ja, jb, jc, :, pl.ds(lane0, ROWS)] = jnp.concatenate([v, v - 1.0], axis=0).astype(BF16)

    def fill_own(m):
        z = m // 2
        for k in range(8):
            y, x = m % 2 * 2 + k // 4, k % 4
            for p in range(3):
                at = ((x, y, z), (y, z, x), (z, x, y))[p]
                put_code(p, *at, 0, turned[z, y, x, core, pl.ds(8 * p, 8), :])

    def fill_other(jj):
        for p in range(3):
            ja = (coord(me, p) + ahead(jj)) % 4
            for jb in range(4):
                for jc in range(4):
                    z, y, x = ((jc, jb, ja), (jb, ja, jc), (ja, jc, jb))[p]
                    put_code(p, ja, jb, jc, ROWS, turned_rx[z, y, x, pl.ds(8 * p, 8), :])

    def other_codes(jj):
        remote(turned_rx.at[0], turned_rx.at[0], pair_send.at[0], pair_recv.at[jj], partner).wait_recv()
        fill_other(jj)

    def turn(m):
        block = raw[m].astype(F32).astype(BF16)
        turned[m // 2, pl.ds(m % 2 * 2, 2)] = block.T.astype(F32).reshape(2, 4, 2, 24, ROWS)

    load(0).wait()
    turn(0)

    @pl.loop(1, LOADS)
    def _(m):
        load(m).wait()
        fill_own(m - 1)
        turn(m)

    for p in range(3):
        pair_copy(0, p).start()

    @pl.loop(0, FEATS // 128)
    def _(k):
        pltpu.make_async_copy(cut_hbm.at[:, pl.ds(k * 128, 128)], cuts.at[k], load_sem.at[LOADS]).start()

    fill_own(LOADS - 1)

    for one in small:
        one.wait()

    def goes_right(j):
        feat = feat_ref[j]
        owner = lax.div(feat, 24)
        bits = [lax.shift_right_logical(owner, k) for k in (5, 3, 1, 0)]
        column = turned[bits[0], bits[1] & 3, bits[2] & 3, bits[3] & 1, pl.ds(feat - 24 * owner, 1), :]
        return (column > thr_ref[j].astype(F32)).astype(jnp.int32)

    leaf = goes_right(0)
    for level in range(1, 5):
        width = 2 ** level
        bit = goes_right(width - 1)
        for n in range(1, width):
            bit = jnp.where(leaf == n, goes_right(width - 1 + n), bit)
        leaf = 2 * leaf + bit
    live = lax.broadcasted_iota(jnp.int32, (1, ROWS), 1) < valid_ref[...]
    grad = jnp.where(live, grad_ref[...], 0.0)
    hess = jnp.where(live, hess_ref[...], 0.0)
    meta[0] = jnp.concatenate([grad, hess, leaf.astype(F32), jnp.zeros((5, ROWS), F32)], axis=0)
    meta_copy.start()
    for jj in range(1, 4):
        for p in range(3):
            pair_copy(jj, p).start()

    def split3(v):
        hi = v.astype(BF16).astype(F32)
        mid = (v - hi).astype(BF16).astype(F32)
        return hi, mid, v - hi - mid

    def fill_weights(side):
        for k in range(ROWS // 128):
            lanes = pl.ds(k * 128, 128)
            g3 = split3(meta[side, 0:1, lanes])
            h3 = split3(meta[side, 1:2, lanes])
            hit = meta[side, 2:3, lanes] == lax.broadcasted_iota(jnp.int32, (LEAVES, 128), 0).astype(F32)
            rows = []
            for i in range(3):
                rows.append(jnp.where(hit, g3[i], 0.0))
                rows.append(jnp.where(hit, h3[i], 0.0))
            rows.append(jnp.zeros((64, 128), F32))
            weights[pl.ds(side * ROWS + k * 128, 128), :] = jnp.concatenate(rows, axis=0).T.astype(BF16)

    fill_weights(0)

    def block(ph, c, p, half, j):
        if ph == 0:
            return hist.at[p, c, j, half]
        return hist.at[p, c, coord(me, p), half, j]

    landings = (rx1, rx2)

    def copy(ph, c, p, kind, half):
        dim = (p + ph) % 3
        at = coord(me, dim)
        step = 1 if (kind == 1) == (half == 1) else -1
        j = (at + 2) % 4 if kind == 0 else (at + step + 4) % 4
        s = ((ph * 2 + c) * 3 + p) * 2 + (0 if kind == 0 else 1)
        return remote(block(ph, c, p, half, j), landings[ph].at[p, c, kind, half], send_sem.at[ph], recv_sem.at[s], neighbour(me, dim, step))

    def wait_landed(ph, c, p, kind, count):
        s = ((ph * 2 + c) * 3 + p) * 2 + (0 if kind == 0 else 1)
        place = landings[ph].at[p, c, pl.ds(kind, count)]
        remote(place, place, send_sem.at[ph], recv_sem.at[s], partner).wait_recv()

    def send_far(ph, c, p):
        copy(ph, c, p, 0, 0).start()
        copy(ph, c, p, 0, 1).start()

    def send_near(ph, c, p):
        copy(ph, c, p, 1, 1).start()
        copy(ph, c, p, 1, 0).start()

    def relay(ph, c, p):
        at = coord(me, (p + ph) % 3)
        wait_landed(ph, c, p, 0, 1)
        for half in range(2):
            mine = block(ph, c, p, half, (at + (1, 3)[half]) % 4)
            mine[...] = mine[...] + landings[ph][p, c, 0, half]
            copy(ph, c, p, 2, half).start()

    def collect(ph, c, p):
        at = coord(me, (p + ph) % 3)
        wait_landed(ph, c, p, 1, 2)
        for half in range(2):
            mine = block(ph, c, p, half, at)
            total = mine[...] + landings[ph][p, c, 1, half] + landings[ph][p, c, 2, half]
            mine[...] = total
        if ph == 0:
            send_far(1, c, p)
            send_near(1, c, p)
        else:
            for step in (2, 1, 3):
                last_copy(c, p, step).start()

    def last_block(c, p, j):
        return hist.at[p, c, coord(me, p), :, coord(me, (p + 1) % 3), pl.ds(2 * j, 2)]

    def last_copy(c, p, step):
        dim = (p + 2) % 3
        j = (coord(me, dim) + step) % 4
        return remote(last_block(c, p, j), rx3.at[p, c, step - 1], send_sem.at[2], recv_sem.at[24 + 3 * c + p], neighbour(me, dim, step))

    def last_collect(c, p):
        remote(rx3.at[p, c], rx3.at[p, c], send_sem.at[2], recv_sem.at[24 + 3 * c + p], partner).wait_recv()
        out_ref[p, c] = last_block(c, p, coord(me, (p + 2) % 3))[...] + rx3[p, c, 0] + rx3[p, c, 1] + rx3[p, c, 2]

    first_half = lax.broadcasted_iota(jnp.int32, (64, 8, 128), 2) < 64

    def unit(c, p, jj, lane0, lanes, add):
        ja = (coord(me, p) + ahead(jj)) % 4
        bounds = [jnp.full((16, lanes), (8 * c + 2 * k).astype(F32), F32).astype(BF16) for k in range(4)]
        one = jnp.asarray(1, BF16)
        zero = jnp.asarray(0, BF16)
        pieces = []
        for half in range(2):
            for jb in range(4):
                for jc in range(4):
                    code = codes2[p, ja, jb, jc, :, pl.ds(lane0, lanes)]
                    for q in range(2):
                        pieces.append(jnp.where(code <= bounds[half * 2 + q], one, zero))
        left = jnp.concatenate(pieces, axis=0)
        sums = jnp.dot(left, weights[pl.ds(lane0, lanes), :], preferred_element_type=F32)
        sums = (sums[:, :128] + sums[:, 128:]).reshape(64, 2, 8, 128)
        even, odd = sums[:, 0], sums[:, 1]
        keep = jnp.where(first_half, even, odd)
        turn = jnp.where(first_half, odd, even).reshape(512, 128)
        both = (keep + pltpu.roll(turn, 64, 1).reshape(64, 8, 128)).reshape(2, 4, 8, 8, 128)
        if add:
            both = both + hist[p, c, ja]
        hist[p, c, ja] = both

    @pl.loop(0, 1 + me // GROUP)
    def _(z):
        for p in range(3):
            unit(z, p, z, 0, ROWS, False)

    other_codes(0)
    meta_copy.wait_recv()
    fill_weights(1)

    def for_parts(task, *args):
        for p in range(3):
            task(*args, p)

    @pl.loop(0, 1 + me // GROUP)
    def _(z):
        for p in range(3):
            unit(z, p, z, ROWS, ROWS, True)

    for_parts(send_far, 0, 0)

    def pick(b, *values):
        return sum((b == k + 1).astype(jnp.int32) * v for k, v in enumerate(values))

    @pl.loop(1, 8)
    def _(b):
        item = (1 - core) * pick(b, 6, 4, 1, 2, 5, 7, 3) + core * pick(b, 4, 5, 6, 1, 2, 7, 3)
        fresh = (1 - core) * pick(b, 1, 0, 1, 0, 0, 1, 0) + core * pick(b, 0, 1, 1, 0, 0, 1, 0)
        c, jj = item // 4, item % 4

        @pl.when(fresh == 1)
        def _():
            other_codes(jj)

        for p in range(3):
            unit(c, p, jj, 0, 2 * ROWS, False)

        @pl.when(jj == 0)
        def _():
            for_parts(send_far, 0, c)

        @pl.when(jj == 1)
        def _():
            for p in range(3):
                copy(0, c, p, 1, 1).start()

        @pl.when(jj == 2)
        def _():
            for p in range(3):
                copy(0, c, p, 1, 0).start()

        @pl.when((core == 0) & (b == 4))
        def _():
            for_parts(relay, 0, 0)

        @pl.when((core == 0) & (b == 5))
        def _():
            for_parts(relay, 0, 1)

        @pl.when((core == 1) & (b == 6))
        def _():
            for_parts(relay, 0, 0)

    pltpu.make_async_copy(cuts, cuts, load_sem.at[LOADS]).wait()
    lanes = lax.broadcasted_iota(jnp.int32, (1, 128), 1)
    steps = lax.broadcasted_iota(jnp.int32, (BINS - 1, 128), 0)
    value = jnp.zeros((1, 128), F32)
    for j in range(INNER):
        feat = feat_ref[j]
        one = jnp.sum(jnp.where(steps == thr_ref[j], cuts[feat // 128], 0.0), axis=0, keepdims=True)
        one = jnp.sum(jnp.where(lanes == feat % 128, one, 0.0), axis=1, keepdims=True)
        value = jnp.where(lanes == j, one, value)
    value_ref[...] = jnp.where(lanes == 127, reg_ref[...], value)

    @pl.when(core == 1)
    def _():
        for_parts(relay, 0, 1)

    for_parts(collect, 0, 0)
    for_parts(collect, 0, 1)
    for_parts(relay, 1, 0)
    for_parts(relay, 1, 1)
    for_parts(collect, 1, 0)
    for_parts(collect, 1, 1)
    for_parts(last_collect, 0)
    for_parts(last_collect, 1)

    meta_copy.wait_send()
    remote(turned_rx, turned_rx, pair_send.at[0], pair_recv.at[4], partner).wait_send()
    for ph, place in enumerate((rx1, rx2, rx3)):
        remote(place, place, send_sem.at[ph], recv_sem.at[0], partner).wait_send()


def gain_kernel(sums_ref, found_ref, gain_ref, leaf_ref, value_ref):
    reg = found_ref[0:1, 127:128]
    sums = sums_ref[...].reshape(192, 128)
    lane = lax.broadcasted_iota(jnp.int32, (128, 256), 0)
    col = lax.broadcasted_iota(jnp.int32, (128, 256), 1)
    same = (lane // 64 == col // 64 % 2) & (lane // 32 % 2 == col // 128)
    under = lane % 32 + 32
    hit = under == col % 64 + 1
    for _ in range(5):
        under = under // 2
        hit = hit | (under == col % 64 + 1)
    pick = jnp.where(same & hit, 1.0, 0.0).astype(BF16)
    hi = sums.astype(BF16)
    rest = sums - hi.astype(F32)
    mid = rest.astype(BF16)
    low = (rest - mid.astype(F32)).astype(BF16)
    nodes = jnp.dot(low, pick, preferred_element_type=F32) + jnp.dot(mid, pick, preferred_element_type=F32) + jnp.dot(hi, pick, preferred_element_type=F32)
    grad = nodes[:, :128].reshape(3, 8, 8, 128)
    hess = nodes[:, 128:].reshape(3, 8, 8, 128)
    upper = lax.broadcasted_iota(jnp.int32, (8, 128), 1) >= 64

    def score(g, h):
        return g * g / (h + reg)

    for p in range(3):
        g_all, h_all = grad[p, 7], hess[p, 7]
        g_all = jnp.where(upper, g_all, pltpu.roll(g_all, 64, 1))
        h_all = jnp.where(upper, h_all, pltpu.roll(h_all, 64, 1))
        whole = score(g_all, h_all)
        for q in range(8):
            g_left, h_left = grad[p, q], hess[p, q]
            gain = 0.5 * (score(g_left, h_left) + score(g_all - g_left, h_all - h_left) - whole)
            gain_ref[2 * q, pl.ds(8 * p, 8), :] = gain[:, :63]
            if q < 7:
                gain_ref[2 * q + 1, pl.ds(8 * p, 8), :] = pltpu.roll(gain, 64, 1)[:, :63]
    last = sums_ref[0, 1, 1, 1]
    g_leaf, h_leaf = pltpu.roll(last, 64, 1), pltpu.roll(last, 32, 1)
    leaf_ref[...] = (-g_leaf / (h_leaf + reg))[0:1, :LEAVES]
    value_ref[...] = found_ref[:, :INNER]


def solution(mesh):
    row_spec = P(('trees', 'data'))
    vmem = pl.BlockSpec(memory_space=pltpu.VMEM)
    hbm = pl.BlockSpec(memory_space=pl.ANY)

    def device_fn(bin_codes, gradient, hessian, valid_rows, split_feat, split_thr, cut_values, reg_lambda):
        sums, found = pl.pallas_call(
            hist_kernel,
            out_shape=(pltpu.VMEM((3, 2, 2, 2, 8, 128), F32), pltpu.VMEM((1, 128), F32)),
            in_specs=[hbm] * 8,
            out_specs=(vmem, vmem),
            scratch_shapes=[
                pltpu.VMEM((1, ROWS), F32),
                pltpu.VMEM((1, ROWS), F32),
                pltpu.VMEM((1, 1), jnp.int32),
                pltpu.SMEM((INNER,), jnp.int32),
                pltpu.SMEM((INNER,), jnp.int32),
                pltpu.VMEM((1, 1), F32),
                pltpu.VMEM((LOADS, ROWS, SLAB), jnp.int32),
                pltpu.VMEM((4, 4, 4, 2, 24, ROWS), F32),
                pltpu.VMEM((4, 4, 4, 24, ROWS), F32),
                pltpu.VMEM((3, 4, 4, 4, 16, 2 * ROWS), BF16),
                pltpu.VMEM((2, 8, ROWS), F32),
                pltpu.VMEM((2 * ROWS, 256), BF16),
                pltpu.VMEM((FEATS // 128, BINS - 1, 128), F32),
                pltpu.VMEM((3, 2, 4, 2, 4, 8, 8, 128), F32),
                pltpu.VMEM((3, 2, 3, 2, 4, 8, 8, 128), F32),
                pltpu.VMEM((3, 2, 3, 2, 8, 8, 128), F32),
                pltpu.VMEM((3, 2, 3, 2, 2, 8, 128), F32),
                pltpu.SemaphoreType.DMA((LOADS + 7,)),
                pltpu.SemaphoreType.DMA((2,)),
                pltpu.SemaphoreType.DMA((5,)),
                pltpu.SemaphoreType.DMA((3,)),
                pltpu.SemaphoreType.DMA((30,)),
            ],
            compiler_params=pltpu.CompilerParams(collective_id=0, has_side_effects=True, vmem_limit_bytes=60 * 1024 * 1024),
            name='hist',
        )(bin_codes, gradient.reshape(1, ROWS), hessian.reshape(1, ROWS), valid_rows.reshape(1, 1), split_feat, split_thr, cut_values.T, reg_lambda.reshape(1, 1))
        gain, leaf, value = pl.pallas_call(
            gain_kernel,
            out_shape=(jax.ShapeDtypeStruct((BINS - 1, FEATS // 128, 63), F32), jax.ShapeDtypeStruct((1, LEAVES), F32), jax.ShapeDtypeStruct((1, INNER), F32)),
            in_specs=[vmem, vmem],
            out_specs=(vmem, vmem, vmem),
            compiler_params=pltpu.CompilerParams(vmem_limit_bytes=4 * 1024 * 1024),
            name='gain',
        )(sums, found)
        return jnp.transpose(gain, (2, 1, 0)), leaf.reshape(LEAVES), value.reshape(INNER)

    return jax.shard_map(device_fn, mesh=mesh, in_specs=(P(('trees', 'data'), None), row_spec, row_spec, row_spec, P('trees'), P('trees'), P('trees', None), P('trees')), out_specs=(P(None, ('trees', 'data'), None), P('trees'), P('trees')), check_vma=False)
```

```python
import functools
import jax
import jax.numpy as jnp
from jax import lax
from jax.experimental import pallas as pl
from jax.experimental.pallas import tpu as pltpu
from jax.sharding import PartitionSpec as P

F32 = jnp.float32
BF16 = jnp.bfloat16
ROWS = 512
FEATS = 3072
BINS = 16
LEAVES = 32
INNER = 31
LOADS = 8
SLAB = FEATS // LOADS
GROUP = 128


def pow4(dim):
    return 1 + 3 * dim * (3 * dim - 1) // 2


def coord(me, dim):
    return (me // 2) // pow4(dim) % 4


def neighbour(me, dim, step):
    at = coord(me, dim)
    return me + ((at + step + 4) % 4 - at) * 2 * pow4(dim)


def hist_kernel(codes_hbm, grad_hbm, hess_hbm, valid_hbm, feat_hbm, thr_hbm, cut_hbm, reg_hbm, out_ref, value_ref,
                grad_ref, hess_ref, valid_ref, feat_ref, thr_ref, reg_ref, raw, turned, turned_rx, codes2, meta, weights, cuts, hist, rx1, rx2, rx3,
                load_sem, pair_send, pair_recv, send_sem, recv_sem):
    me = lax.axis_index('data')
    core = me % 2
    partner = me + 1 - 2 * core

    def remote(src, dst, s_sem, r_sem, device):
        return pltpu.make_async_remote_copy(src_ref=src, dst_ref=dst, send_sem=s_sem, recv_sem=r_sem, device_id=(0, device), device_id_type=pl.DeviceIdType.MESH)

    def load(m):
        return pltpu.make_async_copy(codes_hbm.at[:, pl.ds(m * SLAB, SLAB)], raw.at[m], load_sem.at[m])

    for m in range(LOADS):
        load(m).start()
    small = [pltpu.make_async_copy(src, dst, load_sem.at[LOADS + 1 + k]) for k, (src, dst) in enumerate(
        ((grad_hbm, grad_ref), (hess_hbm, hess_ref), (valid_hbm, valid_ref), (feat_hbm, feat_ref), (thr_hbm, thr_ref), (reg_hbm, reg_ref)))]
    for one in small:
        one.start()
    barrier = pltpu.get_barrier_semaphore()
    pl.semaphore_signal(barrier, inc=1, device_id=(0, partner), device_id_type=pl.DeviceIdType.MESH)
    for dim in range(3):
        for step in (1, 2, 3):
            pl.semaphore_signal(barrier, inc=1, device_id=(0, neighbour(me, dim, step)), device_id_type=pl.DeviceIdType.MESH)

    def ahead(jj):
        return (2 + 3 * jj + (jj // 2) * (7 - 2 * jj)) % 4

    def pair_copy(jj, p):
        ja = (coord(me, p) + ahead(jj)) % 4
        other = 1 - core
        rows = pl.ds(8 * p, 8)
        if p == 0:
            src, dst = turned.at[:, :, ja, other, rows], turned_rx.at[:, :, ja, rows]
        elif p == 1:
            src, dst = turned.at[:, ja, :, other, rows], turned_rx.at[:, ja, :, rows]
        else:
            src, dst = turned.at[ja, :, :, other, rows], turned_rx.at[ja, :, :, rows]
        return remote(src, dst, pair_send.at[0], pair_recv.at[jj], partner)

    meta_copy = remote(meta.at[0], meta.at[1], pair_send.at[1], pair_recv.at[4], partner)

    def put_code(p, ja, jb, jc, lane0, v):
        codes2[p, ja, jb, jc, :, pl.ds(lane0, ROWS)] = jnp.concatenate([v, v - 1.0], axis=0).astype(BF16)

    def fill_own(m):
        z = m // 2
        for k in range(8):
            y, x = m % 2 * 2 + k // 4, k % 4
            for p in range(3):
                at = ((x, y, z), (y, z, x), (z, x, y))[p]
                put_code(p, *at, 0, turned[z, y, x, core, pl.ds(8 * p, 8), :])

    def fill_other(jj):
        for p in range(3):
            ja = (coord(me, p) + ahead(jj)) % 4
            for jb in range(4):
                for jc in range(4):
                    z, y, x = ((jc, jb, ja), (jb, ja, jc), (ja, jc, jb))[p]
                    put_code(p, ja, jb, jc, ROWS, turned_rx[z, y, x, pl.ds(8 * p, 8), :])

    def other_codes(jj):
        remote(turned_rx.at[0], turned_rx.at[0], pair_send.at[0], pair_recv.at[jj], partner).wait_recv()
        fill_other(jj)

    def turn(m):
        block = raw[m].astype(F32).astype(BF16)
        turned[m // 2, pl.ds(m % 2 * 2, 2)] = block.T.astype(F32).reshape(2, 4, 2, 24, ROWS)

    load(0).wait()
    turn(0)

    @pl.loop(1, LOADS)
    def _(m):
        load(m).wait()
        fill_own(m - 1)
        turn(m)

    pl.semaphore_wait(barrier, 10)
    for p in range(3):
        pair_copy(0, p).start()

    @pl.loop(0, FEATS // 128)
    def _(k):
        pltpu.make_async_copy(cut_hbm.at[:, pl.ds(k * 128, 128)], cuts.at[k], load_sem.at[LOADS]).start()

    fill_own(LOADS - 1)

    for one in small:
        one.wait()

    def goes_right(j):
        feat = feat_ref[j]
        owner = lax.div(feat, 24)
        bits = [lax.shift_right_logical(owner, k) for k in (5, 3, 1, 0)]
        column = turned[bits[0], bits[1] & 3, bits[2] & 3, bits[3] & 1, pl.ds(feat - 24 * owner, 1), :]
        return (column > thr_ref[j].astype(F32)).astype(jnp.int32)

    leaf = goes_right(0)
    for level in range(1, 5):
        width = 2 ** level
        bit = goes_right(width - 1)
        for n in range(1, width):
            bit = jnp.where(leaf == n, goes_right(width - 1 + n), bit)
        leaf = 2 * leaf + bit
    live = lax.broadcasted_iota(jnp.int32, (1, ROWS), 1) < valid_ref[...]
    grad = jnp.where(live, grad_ref[...], 0.0)
    hess = jnp.where(live, hess_ref[...], 0.0)
    meta[0] = jnp.concatenate([grad, hess, leaf.astype(F32), jnp.zeros((5, ROWS), F32)], axis=0)
    meta_copy.start()
    for jj in range(1, 4):
        for p in range(3):
            pair_copy(jj, p).start()

    def split3(v):
        hi = v.astype(BF16).astype(F32)
        mid = (v - hi).astype(BF16).astype(F32)
        return hi, mid, v - hi - mid

    def fill_weights(side):
        for k in range(ROWS // 128):
            lanes = pl.ds(k * 128, 128)
            g3 = split3(meta[side, 0:1, lanes])
            h3 = split3(meta[side, 1:2, lanes])
            hit = meta[side, 2:3, lanes] == lax.broadcasted_iota(jnp.int32, (LEAVES, 128), 0).astype(F32)
            rows = []
            for i in range(3):
                rows.append(jnp.where(hit, g3[i], 0.0))
                rows.append(jnp.where(hit, h3[i], 0.0))
            rows.append(jnp.zeros((64, 128), F32))
            weights[pl.ds(side * ROWS + k * 128, 128), :] = jnp.concatenate(rows, axis=0).T.astype(BF16)

    fill_weights(0)

    def block(ph, c, p, half, j):
        if ph == 0:
            return hist.at[p, c, j, half]
        return hist.at[p, c, coord(me, p), half, j]

    landings = (rx1, rx2)

    def copy(ph, c, p, kind, half):
        dim = (p + ph) % 3
        at = coord(me, dim)
        step = 1 if (kind == 1) == (half == 1) else -1
        j = (at + 2) % 4 if kind == 0 else (at + step + 4) % 4
        s = ((ph * 2 + c) * 3 + p) * 2 + (0 if kind == 0 else 1)
        return remote(block(ph, c, p, half, j), landings[ph].at[p, c, kind, half], send_sem.at[ph], recv_sem.at[s], neighbour(me, dim, step))

    def wait_landed(ph, c, p, kind, count):
        s = ((ph * 2 + c) * 3 + p) * 2 + (0 if kind == 0 else 1)
        place = landings[ph].at[p, c, pl.ds(kind, count)]
        remote(place, place, send_sem.at[ph], recv_sem.at[s], partner).wait_recv()

    def send_far(ph, c, p):
        copy(ph, c, p, 0, 0).start()
        copy(ph, c, p, 0, 1).start()

    def send_near(ph, c, p):
        copy(ph, c, p, 1, 1).start()
        copy(ph, c, p, 1, 0).start()

    def relay(ph, c, p):
        at = coord(me, (p + ph) % 3)
        wait_landed(ph, c, p, 0, 1)
        for half in range(2):
            mine = block(ph, c, p, half, (at + (1, 3)[half]) % 4)
            mine[...] = mine[...] + landings[ph][p, c, 0, half]
            copy(ph, c, p, 2, half).start()

    def collect(ph, c, p):
        at = coord(me, (p + ph) % 3)
        wait_landed(ph, c, p, 1, 2)
        for half in range(2):
            mine = block(ph, c, p, half, at)
            total = mine[...] + landings[ph][p, c, 1, half] + landings[ph][p, c, 2, half]
            mine[...] = total
        if ph == 0:
            send_far(1, c, p)
            send_near(1, c, p)
        else:
            for step in (2, 1, 3):
                last_copy(c, p, step).start()

    def last_block(c, p, j):
        return hist.at[p, c, coord(me, p), :, coord(me, (p + 1) % 3), pl.ds(2 * j, 2)]

    def last_copy(c, p, step):
        dim = (p + 2) % 3
        j = (coord(me, dim) + step) % 4
        return remote(last_block(c, p, j), rx3.at[p, c, step - 1], send_sem.at[2], recv_sem.at[24 + 3 * c + p], neighbour(me, dim, step))

    def last_collect(c, p):
        remote(rx3.at[p, c], rx3.at[p, c], send_sem.at[2], recv_sem.at[24 + 3 * c + p], partner).wait_recv()
        out_ref[p, c] = last_block(c, p, coord(me, (p + 2) % 3))[...] + rx3[p, c, 0] + rx3[p, c, 1] + rx3[p, c, 2]

    first_half = lax.broadcasted_iota(jnp.int32, (64, 8, 128), 2) < 64

    def unit(c, p, jj, lane0, lanes, add):
        ja = (coord(me, p) + ahead(jj)) % 4
        bounds = [jnp.full((16, lanes), (8 * c + 2 * k).astype(F32), F32).astype(BF16) for k in range(4)]
        one = jnp.asarray(1, BF16)
        zero = jnp.asarray(0, BF16)
        pieces = []
        for half in range(2):
            for jb in range(4):
                for jc in range(4):
                    code = codes2[p, ja, jb, jc, :, pl.ds(lane0, lanes)]
                    for q in range(2):
                        pieces.append(jnp.where(code <= bounds[half * 2 + q], one, zero))
        left = jnp.concatenate(pieces, axis=0)
        sums = jnp.dot(left, weights[pl.ds(lane0, lanes), :], preferred_element_type=F32)
        sums = (sums[:, :128] + sums[:, 128:]).reshape(64, 2, 8, 128)
        even, odd = sums[:, 0], sums[:, 1]
        keep = jnp.where(first_half, even, odd)
        turn = jnp.where(first_half, odd, even).reshape(512, 128)
        both = (keep + pltpu.roll(turn, 64, 1).reshape(64, 8, 128)).reshape(2, 4, 8, 8, 128)
        if add:
            both = both + hist[p, c, ja]
        hist[p, c, ja] = both

    @pl.loop(0, 1 + me // GROUP)
    def _(z):
        for p in range(3):
            unit(z, p, z, 0, ROWS, False)

    other_codes(0)
    meta_copy.wait_recv()
    fill_weights(1)

    def for_parts(task, *args):
        for p in range(3):
            task(*args, p)

    @pl.loop(0, 1 + me // GROUP)
    def _(z):
        for p in range(3):
            unit(z, p, z, ROWS, ROWS, True)

    for_parts(send_far, 0, 0)

    def pick(b, *values):
        return sum((b == k + 1).astype(jnp.int32) * v for k, v in enumerate(values))

    @pl.loop(1, 8)
    def _(b):
        item = (1 - core) * pick(b, 6, 4, 1, 2, 5, 7, 3) + core * pick(b, 4, 5, 6, 1, 2, 7, 3)
        fresh = (1 - core) * pick(b, 1, 0, 1, 0, 0, 1, 0) + core * pick(b, 0, 1, 1, 0, 0, 1, 0)
        c, jj = item // 4, item % 4

        @pl.when(fresh == 1)
        def _():
            other_codes(jj)

        for p in range(3):
            unit(c, p, jj, 0, 2 * ROWS, False)

        @pl.when(jj == 0)
        def _():
            for_parts(send_far, 0, c)

        @pl.when(jj == 1)
        def _():
            for p in range(3):
                copy(0, c, p, 1, 1).start()

        @pl.when(jj == 2)
        def _():
            for p in range(3):
                copy(0, c, p, 1, 0).start()

        @pl.when((core == 0) & (b == 4))
        def _():
            for_parts(relay, 0, 0)

        @pl.when((core == 0) & (b == 5))
        def _():
            for_parts(relay, 0, 1)

        @pl.when((core == 1) & (b == 6))
        def _():
            for_parts(relay, 0, 0)

    pltpu.make_async_copy(cuts, cuts, load_sem.at[LOADS]).wait()
    lanes = lax.broadcasted_iota(jnp.int32, (1, 128), 1)
    steps = lax.broadcasted_iota(jnp.int32, (BINS - 1, 128), 0)
    value = jnp.zeros((1, 128), F32)
    for j in range(INNER):
        feat = feat_ref[j]
        one = jnp.sum(jnp.where(steps == thr_ref[j], cuts[feat // 128], 0.0), axis=0, keepdims=True)
        one = jnp.sum(jnp.where(lanes == feat % 128, one, 0.0), axis=1, keepdims=True)
        value = jnp.where(lanes == j, one, value)
    value_ref[...] = jnp.where(lanes == 127, reg_ref[...], value)

    @pl.when(core == 1)
    def _():
        for_parts(relay, 0, 1)

    for_parts(collect, 0, 0)
    for_parts(collect, 0, 1)
    for_parts(relay, 1, 0)
    for_parts(relay, 1, 1)
    for_parts(collect, 1, 0)
    for_parts(collect, 1, 1)
    for_parts(last_collect, 0)
    for_parts(last_collect, 1)

    meta_copy.wait_send()
    remote(turned_rx, turned_rx, pair_send.at[0], pair_recv.at[4], partner).wait_send()
    for ph, place in enumerate((rx1, rx2, rx3)):
        remote(place, place, send_sem.at[ph], recv_sem.at[0], partner).wait_send()


def gain_kernel(sums_ref, found_ref, gain_ref, leaf_ref, value_ref):
    reg = found_ref[0:1, 127:128]
    sums = sums_ref[...].reshape(192, 128)
    lane = lax.broadcasted_iota(jnp.int32, (128, 256), 0)
    col = lax.broadcasted_iota(jnp.int32, (128, 256), 1)
    same = (lane // 64 == col // 64 % 2) & (lane // 32 % 2 == col // 128)
    under = lane % 32 + 32
    hit = under == col % 64 + 1
    for _ in range(5):
        under = under // 2
        hit = hit | (under == col % 64 + 1)
    pick = jnp.where(same & hit, 1.0, 0.0).astype(BF16)
    hi = sums.astype(BF16)
    rest = sums - hi.astype(F32)
    mid = rest.astype(BF16)
    low = (rest - mid.astype(F32)).astype(BF16)
    nodes = jnp.dot(low, pick, preferred_element_type=F32) + jnp.dot(mid, pick, preferred_element_type=F32) + jnp.dot(hi, pick, preferred_element_type=F32)
    grad = nodes[:, :128].reshape(3, 8, 8, 128)
    hess = nodes[:, 128:].reshape(3, 8, 8, 128)
    upper = lax.broadcasted_iota(jnp.int32, (8, 128), 1) >= 64

    def score(g, h):
        return g * g / (h + reg)

    for p in range(3):
        g_all, h_all = grad[p, 7], hess[p, 7]
        g_all = jnp.where(upper, g_all, pltpu.roll(g_all, 64, 1))
        h_all = jnp.where(upper, h_all, pltpu.roll(h_all, 64, 1))
        whole = score(g_all, h_all)
        for q in range(8):
            g_left, h_left = grad[p, q], hess[p, q]
            gain = 0.5 * (score(g_left, h_left) + score(g_all - g_left, h_all - h_left) - whole)
            gain_ref[2 * q, pl.ds(8 * p, 8), :] = gain[:, :63]
            if q < 7:
                gain_ref[2 * q + 1, pl.ds(8 * p, 8), :] = pltpu.roll(gain, 64, 1)[:, :63]
    last = sums_ref[0, 1, 1, 1]
    g_leaf, h_leaf = pltpu.roll(last, 64, 1), pltpu.roll(last, 32, 1)
    leaf_ref[...] = (-g_leaf / (h_leaf + reg))[0:1, :LEAVES]
    value_ref[...] = found_ref[:, :INNER]


def solution(mesh):
    row_spec = P(('trees', 'data'))
    vmem = pl.BlockSpec(memory_space=pltpu.VMEM)
    hbm = pl.BlockSpec(memory_space=pl.ANY)

    def device_fn(bin_codes, gradient, hessian, valid_rows, split_feat, split_thr, cut_values, reg_lambda):
        sums, found = pl.pallas_call(
            hist_kernel,
            out_shape=(pltpu.VMEM((3, 2, 2, 2, 8, 128), F32), pltpu.VMEM((1, 128), F32)),
            in_specs=[hbm] * 8,
            out_specs=(vmem, vmem),
            scratch_shapes=[
                pltpu.VMEM((1, ROWS), F32),
                pltpu.VMEM((1, ROWS), F32),
                pltpu.VMEM((1, 1), jnp.int32),
                pltpu.SMEM((INNER,), jnp.int32),
                pltpu.SMEM((INNER,), jnp.int32),
                pltpu.VMEM((1, 1), F32),
                pltpu.VMEM((LOADS, ROWS, SLAB), jnp.int32),
                pltpu.VMEM((4, 4, 4, 2, 24, ROWS), F32),
                pltpu.VMEM((4, 4, 4, 24, ROWS), F32),
                pltpu.VMEM((3, 4, 4, 4, 16, 2 * ROWS), BF16),
                pltpu.VMEM((2, 8, ROWS), F32),
                pltpu.VMEM((2 * ROWS, 256), BF16),
                pltpu.VMEM((FEATS // 128, BINS - 1, 128), F32),
                pltpu.VMEM((3, 2, 4, 2, 4, 8, 8, 128), F32),
                pltpu.VMEM((3, 2, 3, 2, 4, 8, 8, 128), F32),
                pltpu.VMEM((3, 2, 3, 2, 8, 8, 128), F32),
                pltpu.VMEM((3, 2, 3, 2, 2, 8, 128), F32),
                pltpu.SemaphoreType.DMA((LOADS + 7,)),
                pltpu.SemaphoreType.DMA((2,)),
                pltpu.SemaphoreType.DMA((5,)),
                pltpu.SemaphoreType.DMA((3,)),
                pltpu.SemaphoreType.DMA((30,)),
            ],
            compiler_params=pltpu.CompilerParams(collective_id=0, has_side_effects=True, vmem_limit_bytes=60 * 1024 * 1024),
            name='hist',
        )(bin_codes, gradient.reshape(1, ROWS), hessian.reshape(1, ROWS), valid_rows.reshape(1, 1), split_feat, split_thr, cut_values.T, reg_lambda.reshape(1, 1))
        gain, leaf, value = pl.pallas_call(
            gain_kernel,
            out_shape=(jax.ShapeDtypeStruct((BINS - 1, FEATS // 128, 63), F32), jax.ShapeDtypeStruct((1, LEAVES), F32), jax.ShapeDtypeStruct((1, INNER), F32)),
            in_specs=[vmem, vmem],
            out_specs=(vmem, vmem, vmem),
            compiler_params=pltpu.CompilerParams(vmem_limit_bytes=4 * 1024 * 1024),
            name='gain',
        )(sums, found)
        return jnp.transpose(gain, (2, 1, 0)), leaf.reshape(LEAVES), value.reshape(INNER)

    return jax.shard_map(device_fn, mesh=mesh, in_specs=(P(('trees', 'data'), None), row_spec, row_spec, row_spec, P('trees'), P('trees'), P('trees', None), P('trees')), out_specs=(P(None, ('trees', 'data'), None), P('trees'), P('trees')), check_vma=False)
```

```python
import functools
import jax
import jax.numpy as jnp
from jax import lax
from jax.experimental import pallas as pl
from jax.experimental.pallas import tpu as pltpu
from jax.sharding import PartitionSpec as P

F32 = jnp.float32
BF16 = jnp.bfloat16
ROWS = 512
FEATS = 3072
BINS = 16
LEAVES = 32
INNER = 31
LOADS = 8
SLAB = FEATS // LOADS
GROUP = 128


def pow4(dim):
    return 1 + 3 * dim * (3 * dim - 1) // 2


def coord(me, dim):
    return (me // 2) // pow4(dim) % 4


def neighbour(me, dim, step):
    at = coord(me, dim)
    return me + ((at + step + 4) % 4 - at) * 2 * pow4(dim)


def hist_kernel(codes_hbm, grad_hbm, hess_hbm, valid_hbm, feat_hbm, thr_hbm, cut_hbm, reg_hbm, out_ref, value_ref,
                grad_ref, hess_ref, valid_ref, feat_ref, thr_ref, reg_ref, raw, turned, turned_rx, codes2, meta, weights, cuts, hist, rx1, rx2, rx3,
                load_sem, small_sem, pair_recv, recv_sem):
    sent = load_sem
    me = lax.axis_index('data')
    core = me % 2
    partner = me + 1 - 2 * core

    def remote(src, dst, s_sem, r_sem, device):
        return pltpu.make_async_remote_copy(src_ref=src, dst_ref=dst, send_sem=s_sem, recv_sem=r_sem, device_id=(0, device), device_id_type=pl.DeviceIdType.MESH)

    def load(m):
        return pltpu.make_async_copy(codes_hbm.at[:, pl.ds(m * SLAB, SLAB)], raw.at[m], load_sem.at[m])

    for m in range(LOADS):
        load(m).start()
    small = [pltpu.make_async_copy(src, dst, small_sem.at[k]) for k, (src, dst) in enumerate(
        ((grad_hbm, grad_ref), (hess_hbm, hess_ref), (valid_hbm, valid_ref), (feat_hbm, feat_ref), (thr_hbm, thr_ref), (reg_hbm, reg_ref)))]
    for one in small:
        one.start()
    barrier = pltpu.get_barrier_semaphore()
    pl.semaphore_signal(barrier, inc=1, device_id=(0, partner), device_id_type=pl.DeviceIdType.MESH)
    for dim in range(3):
        for step in (1, 2, 3):
            pl.semaphore_signal(barrier, inc=1, device_id=(0, neighbour(me, dim, step)), device_id_type=pl.DeviceIdType.MESH)

    def ahead(jj):
        return (2 + 3 * jj + (jj // 2) * (7 - 2 * jj)) % 4

    def pair_copy(jj, p):
        ja = (coord(me, p) + ahead(jj)) % 4
        other = 1 - core
        rows = pl.ds(8 * p, 8)
        if p == 0:
            src, dst = turned.at[:, :, ja, other, rows], turned_rx.at[:, :, ja, rows]
        elif p == 1:
            src, dst = turned.at[:, ja, :, other, rows], turned_rx.at[:, ja, :, rows]
        else:
            src, dst = turned.at[ja, :, :, other, rows], turned_rx.at[ja, :, :, rows]
        return remote(src, dst, sent.at[3], pair_recv.at[jj], partner)

    meta_copy = remote(meta.at[0], meta.at[1], sent.at[4], pair_recv.at[4], partner)

    def put_code(p, ja, jb, jc, lane0, v):
        codes2[p, ja, jb, jc, :, pl.ds(lane0, ROWS)] = jnp.concatenate([v, v - 1.0], axis=0).astype(BF16)

    def fill_own(m):
        z = m // 2
        for k in range(8):
            y, x = m % 2 * 2 + k // 4, k % 4
            for p in range(3):
                at = ((x, y, z), (y, z, x), (z, x, y))[p]
                put_code(p, *at, 0, turned[z, y, x, core, pl.ds(8 * p, 8), :])

    def fill_other(jj):
        for p in range(3):
            ja = (coord(me, p) + ahead(jj)) % 4
            for jb in range(4):
                for jc in range(4):
                    z, y, x = ((jc, jb, ja), (jb, ja, jc), (ja, jc, jb))[p]
                    put_code(p, ja, jb, jc, ROWS, turned_rx[z, y, x, pl.ds(8 * p, 8), :])

    def other_codes(jj):
        remote(turned_rx.at[0], turned_rx.at[0], sent.at[3], pair_recv.at[jj], partner).wait_recv()
        fill_other(jj)

    def turn(m):
        block = raw[m].astype(F32).astype(BF16)
        turned[m // 2, pl.ds(m % 2 * 2, 2)] = block.T.astype(F32).reshape(2, 4, 2, 24, ROWS)

    load(0).wait()
    turn(0)

    @pl.loop(1, LOADS)
    def _(m):
        load(m).wait()
        fill_own(m - 1)
        turn(m)

    pl.semaphore_wait(barrier, 10)
    for p in range(3):
        pair_copy(0, p).start()

    @pl.loop(0, FEATS // 128)
    def _(k):
        pltpu.make_async_copy(cut_hbm.at[:, pl.ds(k * 128, 128)], cuts.at[k], load_sem.at[5]).start()

    fill_own(LOADS - 1)

    for one in small:
        one.wait()

    def goes_right(j):
        feat = feat_ref[j]
        owner = lax.div(feat, 24)
        bits = [lax.shift_right_logical(owner, k) for k in (5, 3, 1, 0)]
        column = turned[bits[0], bits[1] & 3, bits[2] & 3, bits[3] & 1, pl.ds(feat - 24 * owner, 1), :]
        return (column > thr_ref[j].astype(F32)).astype(jnp.int32)

    leaf = goes_right(0)
    for level in range(1, 5):
        width = 2 ** level
        bit = goes_right(width - 1)
        for n in range(1, width):
            bit = jnp.where(leaf == n, goes_right(width - 1 + n), bit)
        leaf = 2 * leaf + bit
    live = lax.broadcasted_iota(jnp.int32, (1, ROWS), 1) < valid_ref[...]
    grad = jnp.where(live, grad_ref[...], 0.0)
    hess = jnp.where(live, hess_ref[...], 0.0)
    meta[0] = jnp.concatenate([grad, hess, leaf.astype(F32), jnp.zeros((5, ROWS), F32)], axis=0)
    meta_copy.start()
    for jj in range(1, 4):
        for p in range(3):
            pair_copy(jj, p).start()

    def split3(v):
        hi = v.astype(BF16).astype(F32)
        mid = (v - hi).astype(BF16).astype(F32)
        return hi, mid, v - hi - mid

    def fill_weights(side):
        for k in range(ROWS // 128):
            lanes = pl.ds(k * 128, 128)
            g3 = split3(meta[side, 0:1, lanes])
            h3 = split3(meta[side, 1:2, lanes])
            hit = meta[side, 2:3, lanes] == lax.broadcasted_iota(jnp.int32, (LEAVES, 128), 0).astype(F32)
            rows = []
            for i in range(3):
                rows.append(jnp.where(hit, g3[i], 0.0))
                rows.append(jnp.where(hit, h3[i], 0.0))
            rows.append(jnp.zeros((64, 128), F32))
            weights[pl.ds(side * ROWS + k * 128, 128), :] = jnp.concatenate(rows, axis=0).T.astype(BF16)

    fill_weights(0)

    def block(ph, c, p, half, j):
        if ph == 0:
            return hist.at[p, c, j, half]
        return hist.at[p, c, coord(me, p), half, j]

    landings = (rx1, rx2)

    def copy(ph, c, p, kind, half):
        dim = (p + ph) % 3
        at = coord(me, dim)
        step = 1 if (kind == 1) == (half == 1) else -1
        j = (at + 2) % 4 if kind == 0 else (at + step + 4) % 4
        s = (ph * 2 + c) * 2 + (0 if kind == 0 else 1)
        return remote(block(ph, c, p, half, j), landings[ph].at[p, c, kind, half], sent.at[ph], recv_sem.at[s], neighbour(me, dim, step))

    def wait_landed(ph, c, p, kind, count):
        if p == 0:
            place = landings[ph].at[:, c, pl.ds(kind, count)]
            remote(place, place, sent.at[ph], recv_sem.at[(ph * 2 + c) * 2 + (0 if kind == 0 else 1)], partner).wait_recv()

    def send_far(ph, c, p):
        copy(ph, c, p, 0, 0).start()
        copy(ph, c, p, 0, 1).start()

    def send_near(ph, c, p):
        copy(ph, c, p, 1, 1).start()
        copy(ph, c, p, 1, 0).start()

    def relay(ph, c, p):
        at = coord(me, (p + ph) % 3)
        wait_landed(ph, c, p, 0, 1)
        for half in range(2):
            mine = block(ph, c, p, half, (at + (1, 3)[half]) % 4)
            mine[...] = mine[...] + landings[ph][p, c, 0, half]
            copy(ph, c, p, 2, half).start()

    def collect(ph, c, p):
        at = coord(me, (p + ph) % 3)
        wait_landed(ph, c, p, 1, 2)
        for half in range(2):
            mine = block(ph, c, p, half, at)
            total = mine[...] + landings[ph][p, c, 1, half] + landings[ph][p, c, 2, half]
            mine[...] = total
        if ph == 0:
            send_far(1, c, p)
            send_near(1, c, p)
        else:
            for step in (2, 1, 3):
                last_copy(c, p, step).start()

    def last_block(c, p, j):
        return hist.at[p, c, coord(me, p), :, coord(me, (p + 1) % 3), pl.ds(2 * j, 2)]

    def last_copy(c, p, step):
        dim = (p + 2) % 3
        j = (coord(me, dim) + step) % 4
        return remote(last_block(c, p, j), rx3.at[p, c, step - 1], sent.at[2], recv_sem.at[8 + c], neighbour(me, dim, step))

    def last_collect(c, p):
        if p == 0:
            remote(rx3.at[:, c], rx3.at[:, c], sent.at[2], recv_sem.at[8 + c], partner).wait_recv()
        out_ref[p, c] = last_block(c, p, coord(me, (p + 2) % 3))[...] + rx3[p, c, 0] + rx3[p, c, 1] + rx3[p, c, 2]

    first_half = lax.broadcasted_iota(jnp.int32, (64, 8, 128), 2) < 64

    def unit(c, p, jj, lane0, lanes, add):
        ja = (coord(me, p) + ahead(jj)) % 4
        bounds = [jnp.full((16, lanes), (8 * c + 2 * k).astype(F32), F32).astype(BF16) for k in range(4)]
        one = jnp.asarray(1, BF16)
        zero = jnp.asarray(0, BF16)
        pieces = []
        for half in range(2):
            for jb in range(4):
                for jc in range(4):
                    code = codes2[p, ja, jb, jc, :, pl.ds(lane0, lanes)]
                    for q in range(2):
                        pieces.append(jnp.where(code <= bounds[half * 2 + q], one, zero))
        left = jnp.concatenate(pieces, axis=0)
        sums = jnp.dot(left, weights[pl.ds(lane0, lanes), :], preferred_element_type=F32)
        sums = (sums[:, :128] + sums[:, 128:]).reshape(64, 2, 8, 128)
        even, odd = sums[:, 0], sums[:, 1]
        keep = jnp.where(first_half, even, odd)
        turn = jnp.where(first_half, odd, even).reshape(512, 128)
        both = (keep + pltpu.roll(turn, 64, 1).reshape(64, 8, 128)).reshape(2, 4, 8, 8, 128)
        if add:
            both = both + hist[p, c, ja]
        hist[p, c, ja] = both

    @pl.loop(0, 1 + me // GROUP)
    def _(z):
        for p in range(3):
            unit(z, p, z, 0, ROWS, False)

    other_codes(0)
    meta_copy.wait_recv()
    fill_weights(1)

    def for_parts(task, *args):
        for p in range(3):
            task(*args, p)

    @pl.loop(0, 1 + me // GROUP)
    def _(z):
        for p in range(3):
            unit(z, p, z, ROWS, ROWS, True)

    for_parts(send_far, 0, 0)

    def pick(b, *values):
        return sum((b == k + 1).astype(jnp.int32) * v for k, v in enumerate(values))

    @pl.loop(1, 8)
    def _(b):
        item = (1 - core) * pick(b, 6, 4, 1, 2, 5, 7, 3) + core * pick(b, 4, 5, 6, 1, 2, 7, 3)
        fresh = (1 - core) * pick(b, 1, 0, 1, 0, 0, 1, 0) + core * pick(b, 0, 1, 1, 0, 0, 1, 0)
        c, jj = item // 4, item % 4

        @pl.when(fresh == 1)
        def _():
            other_codes(jj)

        for p in range(3):
            unit(c, p, jj, 0, 2 * ROWS, False)

        @pl.when(jj == 0)
        def _():
            for_parts(send_far, 0, c)

        @pl.when(jj == 1)
        def _():
            for p in range(3):
                copy(0, c, p, 1, 1).start()

        @pl.when(jj == 2)
        def _():
            for p in range(3):
                copy(0, c, p, 1, 0).start()

        @pl.when((core == 0) & (b == 4))
        def _():
            for_parts(relay, 0, 0)

        @pl.when((core == 0) & (b == 5))
        def _():
            for_parts(relay, 0, 1)

        @pl.when((core == 1) & (b == 6))
        def _():
            for_parts(relay, 0, 0)

    pltpu.make_async_copy(cuts, cuts, load_sem.at[5]).wait()
    lanes = lax.broadcasted_iota(jnp.int32, (1, 128), 1)
    steps = lax.broadcasted_iota(jnp.int32, (BINS - 1, 128), 0)
    value = jnp.zeros((1, 128), F32)
    for j in range(INNER):
        feat = feat_ref[j]
        one = jnp.sum(jnp.where(steps == thr_ref[j], cuts[feat // 128], 0.0), axis=0, keepdims=True)
        one = jnp.sum(jnp.where(lanes == feat % 128, one, 0.0), axis=1, keepdims=True)
        value = jnp.where(lanes == j, one, value)
    value_ref[...] = jnp.where(lanes == 127, reg_ref[...], value)

    @pl.when(core == 1)
    def _():
        for_parts(relay, 0, 1)

    for_parts(collect, 0, 0)
    for_parts(collect, 0, 1)
    for_parts(relay, 1, 0)
    for_parts(relay, 1, 1)
    for_parts(collect, 1, 0)
    for_parts(collect, 1, 1)
    for_parts(last_collect, 0)
    for_parts(last_collect, 1)

    meta_copy.wait_send()
    remote(turned_rx, turned_rx, sent.at[3], pair_recv.at[4], partner).wait_send()
    for ph, place in enumerate((rx1, rx2, rx3)):
        remote(place, place, sent.at[ph], recv_sem.at[0], partner).wait_send()


def gain_kernel(sums_ref, found_ref, gain_ref, leaf_ref, value_ref):
    reg = found_ref[0:1, 127:128]
    sums = sums_ref[...].reshape(192, 128)
    lane = lax.broadcasted_iota(jnp.int32, (128, 256), 0)
    col = lax.broadcasted_iota(jnp.int32, (128, 256), 1)
    same = (lane // 64 == col // 64 % 2) & (lane // 32 % 2 == col // 128)
    under = lane % 32 + 32
    hit = under == col % 64 + 1
    for _ in range(5):
        under = under // 2
        hit = hit | (under == col % 64 + 1)
    pick = jnp.where(same & hit, 1.0, 0.0).astype(BF16)
    hi = sums.astype(BF16)
    rest = sums - hi.astype(F32)
    mid = rest.astype(BF16)
    low = (rest - mid.astype(F32)).astype(BF16)
    nodes = jnp.dot(low, pick, preferred_element_type=F32) + jnp.dot(mid, pick, preferred_element_type=F32) + jnp.dot(hi, pick, preferred_element_type=F32)
    grad = nodes[:, :128].reshape(3, 8, 8, 128)
    hess = nodes[:, 128:].reshape(3, 8, 8, 128)
    upper = lax.broadcasted_iota(jnp.int32, (8, 128), 1) >= 64

    def score(g, h):
        return g * g / (h + reg)

    for p in range(3):
        g_all, h_all = grad[p, 7], hess[p, 7]
        g_all = jnp.where(upper, g_all, pltpu.roll(g_all, 64, 1))
        h_all = jnp.where(upper, h_all, pltpu.roll(h_all, 64, 1))
        whole = score(g_all, h_all)
        for q in range(8):
            g_left, h_left = grad[p, q], hess[p, q]
            gain = 0.5 * (score(g_left, h_left) + score(g_all - g_left, h_all - h_left) - whole)
            gain_ref[2 * q, pl.ds(8 * p, 8), :] = gain[:, :63]
            if q < 7:
                gain_ref[2 * q + 1, pl.ds(8 * p, 8), :] = pltpu.roll(gain, 64, 1)[:, :63]
    last = sums_ref[0, 1, 1, 1]
    g_leaf, h_leaf = pltpu.roll(last, 64, 1), pltpu.roll(last, 32, 1)
    leaf_ref[...] = (-g_leaf / (h_leaf + reg))[0:1, :LEAVES]
    value_ref[...] = found_ref[:, :INNER]


def solution(mesh):
    row_spec = P(('trees', 'data'))
    vmem = pl.BlockSpec(memory_space=pltpu.VMEM)
    hbm = pl.BlockSpec(memory_space=pl.ANY)

    def device_fn(bin_codes, gradient, hessian, valid_rows, split_feat, split_thr, cut_values, reg_lambda):
        sums, found = pl.pallas_call(
            hist_kernel,
            out_shape=(pltpu.VMEM((3, 2, 2, 2, 8, 128), F32), pltpu.VMEM((1, 128), F32)),
            in_specs=[hbm] * 8,
            out_specs=(vmem, vmem),
            scratch_shapes=[
                pltpu.VMEM((1, ROWS), F32),
                pltpu.VMEM((1, ROWS), F32),
                pltpu.VMEM((1, 1), jnp.int32),
                pltpu.SMEM((INNER,), jnp.int32),
                pltpu.SMEM((INNER,), jnp.int32),
                pltpu.VMEM((1, 1), F32),
                pltpu.VMEM((LOADS, ROWS, SLAB), jnp.int32),
                pltpu.VMEM((4, 4, 4, 2, 24, ROWS), F32),
                pltpu.VMEM((4, 4, 4, 24, ROWS), F32),
                pltpu.VMEM((3, 4, 4, 4, 16, 2 * ROWS), BF16),
                pltpu.VMEM((2, 8, ROWS), F32),
                pltpu.VMEM((2 * ROWS, 256), BF16),
                pltpu.VMEM((FEATS // 128, BINS - 1, 128), F32),
                pltpu.VMEM((3, 2, 4, 2, 4, 8, 8, 128), F32),
                pltpu.VMEM((3, 2, 3, 2, 4, 8, 8, 128), F32),
                pltpu.VMEM((3, 2, 3, 2, 8, 8, 128), F32),
                pltpu.VMEM((3, 2, 3, 2, 2, 8, 128), F32),
                pltpu.SemaphoreType.DMA((LOADS,)),
                pltpu.SemaphoreType.DMA((6,)),
                pltpu.SemaphoreType.DMA((5,)),
                pltpu.SemaphoreType.DMA((10,)),
            ],
            compiler_params=pltpu.CompilerParams(collective_id=0, has_side_effects=True, vmem_limit_bytes=60 * 1024 * 1024),
            name='hist',
        )(bin_codes, gradient.reshape(1, ROWS), hessian.reshape(1, ROWS), valid_rows.reshape(1, 1), split_feat, split_thr, cut_values.T, reg_lambda.reshape(1, 1))
        gain, leaf, value = pl.pallas_call(
            gain_kernel,
            out_shape=(jax.ShapeDtypeStruct((BINS - 1, FEATS // 128, 63), F32), jax.ShapeDtypeStruct((1, LEAVES), F32), jax.ShapeDtypeStruct((1, INNER), F32)),
            in_specs=[vmem, vmem],
            out_specs=(vmem, vmem, vmem),
            compiler_params=pltpu.CompilerParams(vmem_limit_bytes=4 * 1024 * 1024),
            name='gain',
        )(sums, found)
        return jnp.transpose(gain, (2, 1, 0)), leaf.reshape(LEAVES), value.reshape(INNER)

    return jax.shard_map(device_fn, mesh=mesh, in_specs=(P(('trees', 'data'), None), row_spec, row_spec, row_spec, P('trees'), P('trees'), P('trees', None), P('trees')), out_specs=(P(None, ('trees', 'data'), None), P('trees'), P('trees')), check_vma=False)
```

```python
import functools
import jax
import jax.numpy as jnp
from jax import lax
from jax.experimental import pallas as pl
from jax.experimental.pallas import tpu as pltpu
from jax.sharding import PartitionSpec as P

F32 = jnp.float32
BF16 = jnp.bfloat16
ROWS = 512
FEATS = 3072
BINS = 16
LEAVES = 32
INNER = 31
LOADS = 8
SLAB = FEATS // LOADS
GROUP = 128


def pow4(dim):
    return 1 + 3 * dim * (3 * dim - 1) // 2


def coord(me, dim):
    return (me // 2) // pow4(dim) % 4


def neighbour(me, dim, step):
    at = coord(me, dim)
    return me + ((at + step + 4) % 4 - at) * 2 * pow4(dim)


def hist_kernel(codes_hbm, grad_hbm, hess_hbm, valid_hbm, feat_hbm, thr_hbm, cut_hbm, reg_hbm, out_ref, value_ref,
                grad_ref, hess_ref, valid_ref, feat_ref, thr_ref, reg_ref, raw, turned, turned_rx, codes2, meta, weights, cuts, hist, rx1, rx2, rx3,
                load_sem, small_sem, pair_recv, recv_sem):
    sent = load_sem
    me = lax.axis_index('data')
    core = me % 2
    partner = me + 1 - 2 * core

    def remote(src, dst, s_sem, r_sem, device):
        return pltpu.make_async_remote_copy(src_ref=src, dst_ref=dst, send_sem=s_sem, recv_sem=r_sem, device_id=(0, device), device_id_type=pl.DeviceIdType.MESH)

    first = 2 * ((coord(me, 2) + 2) % 4)

    def load(m):
        return pltpu.make_async_copy(codes_hbm.at[:, pl.ds((m + first) % LOADS * SLAB, SLAB)], raw.at[m], load_sem.at[m])

    for m in range(LOADS):
        load(m).start()
    small = [pltpu.make_async_copy(src, dst, small_sem.at[k]) for k, (src, dst) in enumerate(
        ((grad_hbm, grad_ref), (hess_hbm, hess_ref), (valid_hbm, valid_ref), (feat_hbm, feat_ref), (thr_hbm, thr_ref), (reg_hbm, reg_ref)))]
    for one in small:
        one.start()
    barrier = pltpu.get_barrier_semaphore()
    pl.semaphore_signal(barrier, inc=1, device_id=(0, partner), device_id_type=pl.DeviceIdType.MESH)
    for dim in range(3):
        for step in (1, 2, 3):
            pl.semaphore_signal(barrier, inc=1, device_id=(0, neighbour(me, dim, step)), device_id_type=pl.DeviceIdType.MESH)

    def ahead(jj):
        return (2 + 3 * jj + (jj // 2) * (7 - 2 * jj)) % 4

    def pair_copy(jj, p):
        ja = (coord(me, p) + ahead(jj)) % 4
        other = 1 - core
        rows = pl.ds(8 * p, 8)
        if p == 0:
            src, dst = turned.at[:, :, ja, other, rows], turned_rx.at[:, :, ja, rows]
        elif p == 1:
            src, dst = turned.at[:, ja, :, other, rows], turned_rx.at[:, ja, :, rows]
        else:
            src, dst = turned.at[ja, :, :, other, rows], turned_rx.at[ja, :, :, rows]
        return remote(src, dst, small_sem.at[6], pair_recv.at[jj], partner)

    meta_copy = remote(meta.at[0], meta.at[1], sent.at[4], pair_recv.at[4], partner)

    def put_code(p, ja, jb, jc, lane0, v):
        codes2[p, ja, jb, jc, :, pl.ds(lane0, ROWS)] = jnp.concatenate([v, v - 1.0], axis=0).astype(BF16)

    def fill_own(m):
        m = (m + first) % LOADS
        z = m // 2
        for k in range(8):
            y, x = m % 2 * 2 + k // 4, k % 4
            for p in range(3):
                at = ((x, y, z), (y, z, x), (z, x, y))[p]
                put_code(p, *at, 0, turned[z, y, x, core, pl.ds(8 * p, 8), :])

    def fill_other(jj):
        for p in range(3):
            ja = (coord(me, p) + ahead(jj)) % 4
            for jb in range(4):
                for jc in range(4):
                    z, y, x = ((jc, jb, ja), (jb, ja, jc), (ja, jc, jb))[p]
                    put_code(p, ja, jb, jc, ROWS, turned_rx[z, y, x, pl.ds(8 * p, 8), :])

    def other_codes(jj):
        remote(turned_rx.at[0], turned_rx.at[0], small_sem.at[6], pair_recv.at[jj], partner).wait_recv()
        fill_other(jj)

    def turn(m):
        block = raw[m].astype(F32).astype(BF16)
        at = (m + first) % LOADS
        turned[at // 2, pl.ds(at % 2 * 2, 2)] = block.T.astype(F32).reshape(2, 4, 2, 24, ROWS)

    load(0).wait()
    turn(0)

    @pl.loop(1, LOADS)
    def _(m):
        load(m).wait()
        fill_own(m - 1)
        turn(m)

        @pl.when(m == 3)
        def _():
            pl.semaphore_wait(barrier, 10)
            pair_copy(0, 2).start()

    for p in range(2):
        pair_copy(0, p).start()

    @pl.loop(0, FEATS // 128)
    def _(k):
        pltpu.make_async_copy(cut_hbm.at[:, pl.ds(k * 128, 128)], cuts.at[k], load_sem.at[5]).start()

    fill_own(LOADS - 1)

    for one in small:
        one.wait()

    def goes_right(j):
        feat = feat_ref[j]
        owner = lax.div(feat, 24)
        bits = [lax.shift_right_logical(owner, k) for k in (5, 3, 1, 0)]
        column = turned[bits[0], bits[1] & 3, bits[2] & 3, bits[3] & 1, pl.ds(feat - 24 * owner, 1), :]
        return (column > thr_ref[j].astype(F32)).astype(jnp.int32)

    leaf = goes_right(0)
    for level in range(1, 5):
        width = 2 ** level
        bit = goes_right(width - 1)
        for n in range(1, width):
            bit = jnp.where(leaf == n, goes_right(width - 1 + n), bit)
        leaf = 2 * leaf + bit
    live = lax.broadcasted_iota(jnp.int32, (1, ROWS), 1) < valid_ref[...]
    grad = jnp.where(live, grad_ref[...], 0.0)
    hess = jnp.where(live, hess_ref[...], 0.0)
    meta[0] = jnp.concatenate([grad, hess, leaf.astype(F32), jnp.zeros((5, ROWS), F32)], axis=0)
    meta_copy.start()
    for jj in range(1, 4):
        for p in range(3):
            pair_copy(jj, p).start()

    def split3(v):
        hi = v.astype(BF16).astype(F32)
        mid = (v - hi).astype(BF16).astype(F32)
        return hi, mid, v - hi - mid

    def fill_weights(side):
        for k in range(ROWS // 128):
            lanes = pl.ds(k * 128, 128)
            g3 = split3(meta[side, 0:1, lanes])
            h3 = split3(meta[side, 1:2, lanes])
            hit = meta[side, 2:3, lanes] == lax.broadcasted_iota(jnp.int32, (LEAVES, 128), 0).astype(F32)
            rows = []
            for i in range(3):
                rows.append(jnp.where(hit, g3[i], 0.0))
                rows.append(jnp.where(hit, h3[i], 0.0))
            rows.append(jnp.zeros((64, 128), F32))
            weights[pl.ds(side * ROWS + k * 128, 128), :] = jnp.concatenate(rows, axis=0).T.astype(BF16)

    fill_weights(0)

    def block(ph, c, p, half, j):
        if ph == 0:
            return hist.at[p, c, j, half]
        return hist.at[p, c, coord(me, p), half, j]

    landings = (rx1, rx2)

    def copy(ph, c, p, kind, half):
        dim = (p + ph) % 3
        at = coord(me, dim)
        step = 1 if (kind == 1) == (half == 1) else -1
        j = (at + 2) % 4 if kind == 0 else (at + step + 4) % 4
        s = (ph * 2 + c) * 2 + (0 if kind == 0 else 1)
        return remote(block(ph, c, p, half, j), landings[ph].at[p, c, kind, half], sent.at[ph], recv_sem.at[s], neighbour(me, dim, step))

    def wait_landed(ph, c, p, kind, count):
        if p == 0:
            place = landings[ph].at[:, c, pl.ds(kind, count)]
            remote(place, place, sent.at[ph], recv_sem.at[(ph * 2 + c) * 2 + (0 if kind == 0 else 1)], partner).wait_recv()

    def send_far(ph, c, p):
        copy(ph, c, p, 0, 0).start()
        copy(ph, c, p, 0, 1).start()

    def send_near(ph, c, p):
        copy(ph, c, p, 1, 1).start()
        copy(ph, c, p, 1, 0).start()

    def relay(ph, c, p):
        at = coord(me, (p + ph) % 3)
        wait_landed(ph, c, p, 0, 1)
        for half in range(2):
            mine = block(ph, c, p, half, (at + (1, 3)[half]) % 4)
            mine[...] = mine[...] + landings[ph][p, c, 0, half]
            copy(ph, c, p, 2, half).start()

    def collect(ph, c, p):
        at = coord(me, (p + ph) % 3)
        wait_landed(ph, c, p, 1, 2)
        for half in range(2):
            mine = block(ph, c, p, half, at)
            total = mine[...] + landings[ph][p, c, 1, half] + landings[ph][p, c, 2, half]
            mine[...] = total
        if ph == 0:
            send_far(1, c, p)
            send_near(1, c, p)
        else:
            for step in (2, 1, 3):
                last_copy(c, p, step).start()

    def last_block(c, p, j):
        return hist.at[p, c, coord(me, p), :, coord(me, (p + 1) % 3), pl.ds(2 * j, 2)]

    def last_copy(c, p, step):
        dim = (p + 2) % 3
        j = (coord(me, dim) + step) % 4
        return remote(last_block(c, p, j), rx3.at[p, c, step - 1], sent.at[2], recv_sem.at[8 + c], neighbour(me, dim, step))

    def last_collect(c, p):
        if p == 0:
            remote(rx3.at[:, c], rx3.at[:, c], sent.at[2], recv_sem.at[8 + c], partner).wait_recv()
        out_ref[p, c] = last_block(c, p, coord(me, (p + 2) % 3))[...] + rx3[p, c, 0] + rx3[p, c, 1] + rx3[p, c, 2]

    first_half = lax.broadcasted_iota(jnp.int32, (64, 8, 128), 2) < 64

    def unit(c, p, jj, lane0, lanes, add):
        ja = (coord(me, p) + ahead(jj)) % 4
        bounds = [jnp.full((16, lanes), (8 * c + 2 * k).astype(F32), F32).astype(BF16) for k in range(4)]
        one = jnp.asarray(1, BF16)
        zero = jnp.asarray(0, BF16)
        pieces = []
        for half in range(2):
            for jb in range(4):
                for jc in range(4):
                    code = codes2[p, ja, jb, jc, :, pl.ds(lane0, lanes)]
                    for q in range(2):
                        pieces.append(jnp.where(code <= bounds[half * 2 + q], one, zero))
        left = jnp.concatenate(pieces, axis=0)
        sums = jnp.dot(left, weights[pl.ds(lane0, lanes), :], preferred_element_type=F32)
        sums = (sums[:, :128] + sums[:, 128:]).reshape(64, 2, 8, 128)
        even, odd = sums[:, 0], sums[:, 1]
        keep = jnp.where(first_half, even, odd)
        turn = jnp.where(first_half, odd, even).reshape(512, 128)
        both = (keep + pltpu.roll(turn, 64, 1).reshape(64, 8, 128)).reshape(2, 4, 8, 8, 128)
        if add:
            both = both + hist[p, c, ja]
        hist[p, c, ja] = both

    @pl.loop(0, 1 + me // GROUP)
    def _(z):
        for p in range(3):
            unit(z, p, z, 0, ROWS, False)

    other_codes(0)
    meta_copy.wait_recv()
    fill_weights(1)

    def for_parts(task, *args):
        for p in range(3):
            task(*args, p)

    @pl.loop(0, 1 + me // GROUP)
    def _(z):
        for p in range(3):
            unit(z, p, z, ROWS, ROWS, True)

    for_parts(send_far, 0, 0)

    def pick(b, *values):
        return sum((b == k + 1).astype(jnp.int32) * v for k, v in enumerate(values))

    @pl.loop(1, 8)
    def _(b):
        item = (1 - core) * pick(b, 6, 4, 1, 2, 5, 7, 3) + core * pick(b, 4, 5, 6, 1, 2, 7, 3)
        fresh = (1 - core) * pick(b, 1, 0, 1, 0, 0, 1, 0) + core * pick(b, 0, 1, 1, 0, 0, 1, 0)
        c, jj = item // 4, item % 4

        @pl.when(fresh == 1)
        def _():
            other_codes(jj)

        for p in range(3):
            unit(c, p, jj, 0, 2 * ROWS, False)

        @pl.when(jj == 0)
        def _():
            for_parts(send_far, 0, c)

        @pl.when(jj == 1)
        def _():
            for p in range(3):
                copy(0, c, p, 1, 1).start()

        @pl.when(jj == 2)
        def _():
            for p in range(3):
                copy(0, c, p, 1, 0).start()

        @pl.when((core == 0) & (b == 4))
        def _():
            for_parts(relay, 0, 0)

        @pl.when((core == 0) & (b == 5))
        def _():
            for_parts(relay, 0, 1)

        @pl.when((core == 1) & (b == 6))
        def _():
            for_parts(relay, 0, 0)

    pltpu.make_async_copy(cuts, cuts, load_sem.at[5]).wait()
    lanes = lax.broadcasted_iota(jnp.int32, (1, 128), 1)
    steps = lax.broadcasted_iota(jnp.int32, (BINS - 1, 128), 0)
    value = jnp.zeros((1, 128), F32)
    for j in range(INNER):
        feat = feat_ref[j]
        one = jnp.sum(jnp.where(steps == thr_ref[j], cuts[feat // 128], 0.0), axis=0, keepdims=True)
        one = jnp.sum(jnp.where(lanes == feat % 128, one, 0.0), axis=1, keepdims=True)
        value = jnp.where(lanes == j, one, value)
    value_ref[...] = jnp.where(lanes == 127, reg_ref[...], value)

    @pl.when(core == 1)
    def _():
        for_parts(relay, 0, 1)

    for_parts(collect, 0, 0)
    for_parts(collect, 0, 1)
    for_parts(relay, 1, 0)
    for_parts(relay, 1, 1)
    for_parts(collect, 1, 0)
    for_parts(collect, 1, 1)
    for_parts(last_collect, 0)
    for_parts(last_collect, 1)

    meta_copy.wait_send()
    remote(turned_rx, turned_rx, small_sem.at[6], pair_recv.at[4], partner).wait_send()
    for ph, place in enumerate((rx1, rx2, rx3)):
        remote(place, place, sent.at[ph], recv_sem.at[0], partner).wait_send()


def gain_kernel(sums_ref, found_ref, gain_ref, leaf_ref, value_ref):
    reg = found_ref[0:1, 127:128]
    sums = sums_ref[...].reshape(192, 128)
    lane = lax.broadcasted_iota(jnp.int32, (128, 256), 0)
    col = lax.broadcasted_iota(jnp.int32, (128, 256), 1)
    same = (lane // 64 == col // 64 % 2) & (lane // 32 % 2 == col // 128)
    under = lane % 32 + 32
    hit = under == col % 64 + 1
    for _ in range(5):
        under = under // 2
        hit = hit | (under == col % 64 + 1)
    pick = jnp.where(same & hit, 1.0, 0.0).astype(BF16)
    hi = sums.astype(BF16)
    rest = sums - hi.astype(F32)
    mid = rest.astype(BF16)
    low = (rest - mid.astype(F32)).astype(BF16)
    nodes = jnp.dot(low, pick, preferred_element_type=F32) + jnp.dot(mid, pick, preferred_element_type=F32) + jnp.dot(hi, pick, preferred_element_type=F32)
    grad = nodes[:, :128].reshape(3, 8, 8, 128)
    hess = nodes[:, 128:].reshape(3, 8, 8, 128)
    upper = lax.broadcasted_iota(jnp.int32, (8, 128), 1) >= 64

    def score(g, h):
        return g * g / (h + reg)

    for p in range(3):
        g_all, h_all = grad[p, 7], hess[p, 7]
        g_all = jnp.where(upper, g_all, pltpu.roll(g_all, 64, 1))
        h_all = jnp.where(upper, h_all, pltpu.roll(h_all, 64, 1))
        whole = score(g_all, h_all)
        for q in range(8):
            g_left, h_left = grad[p, q], hess[p, q]
            gain = 0.5 * (score(g_left, h_left) + score(g_all - g_left, h_all - h_left) - whole)
            gain_ref[2 * q, pl.ds(8 * p, 8), :] = gain[:, :63]
            if q < 7:
                gain_ref[2 * q + 1, pl.ds(8 * p, 8), :] = pltpu.roll(gain, 64, 1)[:, :63]
    last = sums_ref[0, 1, 1, 1]
    g_leaf, h_leaf = pltpu.roll(last, 64, 1), pltpu.roll(last, 32, 1)
    leaf_ref[...] = (-g_leaf / (h_leaf + reg))[0:1, :LEAVES]
    value_ref[...] = found_ref[:, :INNER]


def solution(mesh):
    row_spec = P(('trees', 'data'))
    vmem = pl.BlockSpec(memory_space=pltpu.VMEM)
    hbm = pl.BlockSpec(memory_space=pl.ANY)

    def device_fn(bin_codes, gradient, hessian, valid_rows, split_feat, split_thr, cut_values, reg_lambda):
        sums, found = pl.pallas_call(
            hist_kernel,
            out_shape=(pltpu.VMEM((3, 2, 2, 2, 8, 128), F32), pltpu.VMEM((1, 128), F32)),
            in_specs=[hbm] * 8,
            out_specs=(vmem, vmem),
            scratch_shapes=[
                pltpu.VMEM((1, ROWS), F32),
                pltpu.VMEM((1, ROWS), F32),
                pltpu.VMEM((1, 1), jnp.int32),
                pltpu.SMEM((INNER,), jnp.int32),
                pltpu.SMEM((INNER,), jnp.int32),
                pltpu.VMEM((1, 1), F32),
                pltpu.VMEM((LOADS, ROWS, SLAB), jnp.int32),
                pltpu.VMEM((4, 4, 4, 2, 24, ROWS), F32),
                pltpu.VMEM((4, 4, 4, 24, ROWS), F32),
                pltpu.VMEM((3, 4, 4, 4, 16, 2 * ROWS), BF16),
                pltpu.VMEM((2, 8, ROWS), F32),
                pltpu.VMEM((2 * ROWS, 256), BF16),
                pltpu.VMEM((FEATS // 128, BINS - 1, 128), F32),
                pltpu.VMEM((3, 2, 4, 2, 4, 8, 8, 128), F32),
                pltpu.VMEM((3, 2, 3, 2, 4, 8, 8, 128), F32),
                pltpu.VMEM((3, 2, 3, 2, 8, 8, 128), F32),
                pltpu.VMEM((3, 2, 3, 2, 2, 8, 128), F32),
                pltpu.SemaphoreType.DMA((LOADS,)),
                pltpu.SemaphoreType.DMA((7,)),
                pltpu.SemaphoreType.DMA((5,)),
                pltpu.SemaphoreType.DMA((10,)),
            ],
            compiler_params=pltpu.CompilerParams(collective_id=0, has_side_effects=True, vmem_limit_bytes=60 * 1024 * 1024),
            name='hist',
        )(bin_codes, gradient.reshape(1, ROWS), hessian.reshape(1, ROWS), valid_rows.reshape(1, 1), split_feat, split_thr, cut_values.T, reg_lambda.reshape(1, 1))
        gain, leaf, value = pl.pallas_call(
            gain_kernel,
            out_shape=(jax.ShapeDtypeStruct((BINS - 1, FEATS // 128, 63), F32), jax.ShapeDtypeStruct((1, LEAVES), F32), jax.ShapeDtypeStruct((1, INNER), F32)),
            in_specs=[vmem, vmem],
            out_specs=(vmem, vmem, vmem),
            compiler_params=pltpu.CompilerParams(vmem_limit_bytes=4 * 1024 * 1024),
            name='gain',
        )(sums, found)
        return jnp.transpose(gain, (2, 1, 0)), leaf.reshape(LEAVES), value.reshape(INNER)

    return jax.shard_map(device_fn, mesh=mesh, in_specs=(P(('trees', 'data'), None), row_spec, row_spec, row_spec, P('trees'), P('trees'), P('trees', None), P('trees')), out_specs=(P(None, ('trees', 'data'), None), P('trees'), P('trees')), check_vma=False)
```

```python
import functools
import jax
import jax.numpy as jnp
from jax import lax
from jax.experimental import pallas as pl
from jax.experimental.pallas import tpu as pltpu
from jax.sharding import PartitionSpec as P

F32 = jnp.float32
BF16 = jnp.bfloat16
ROWS = 512
FEATS = 3072
BINS = 16
LEAVES = 32
INNER = 31
LOADS = 8
SLAB = FEATS // LOADS
GROUP = 128


def pow4(dim):
    return 1 + 3 * dim * (3 * dim - 1) // 2


def coord(me, dim):
    return (me // 2) // pow4(dim) % 4


def neighbour(me, dim, step):
    at = coord(me, dim)
    return me + ((at + step + 4) % 4 - at) * 2 * pow4(dim)


def hist_kernel(codes_hbm, grad_hbm, hess_hbm, valid_hbm, feat_hbm, thr_hbm, cut_hbm, reg_hbm, out_ref, value_ref,
                grad_ref, hess_ref, valid_ref, feat_ref, thr_ref, reg_ref, raw, turned, turned_rx, codes2, meta, weights, cuts, hist, rx1, rx2, rx3,
                load_sem, small_sem, pair_recv, recv_sem):
    sent = load_sem
    me = lax.axis_index('data')
    core = me % 2
    partner = me + 1 - 2 * core

    def remote(src, dst, s_sem, r_sem, device):
        return pltpu.make_async_remote_copy(src_ref=src, dst_ref=dst, send_sem=s_sem, recv_sem=r_sem, device_id=(0, device), device_id_type=pl.DeviceIdType.MESH)

    first = 2 * ((coord(me, 2) + 2) % 4)

    def load(m):
        return pltpu.make_async_copy(codes_hbm.at[:, pl.ds((m + first) % LOADS * SLAB, SLAB)], raw.at[m], load_sem.at[m])

    for m in range(LOADS):
        load(m).start()
    small = [pltpu.make_async_copy(src, dst, small_sem.at[k]) for k, (src, dst) in enumerate(
        ((grad_hbm, grad_ref), (hess_hbm, hess_ref), (valid_hbm, valid_ref), (feat_hbm, feat_ref), (thr_hbm, thr_ref), (reg_hbm, reg_ref)))]
    for one in small:
        one.start()
    barrier = pltpu.get_barrier_semaphore()
    pl.semaphore_signal(barrier, inc=1, device_id=(0, partner), device_id_type=pl.DeviceIdType.MESH)
    for dim in range(3):
        for step in (1, 2, 3):
            pl.semaphore_signal(barrier, inc=1, device_id=(0, neighbour(me, dim, step)), device_id_type=pl.DeviceIdType.MESH)

    def ahead(jj):
        return (2 + 3 * jj + (jj // 2) * (7 - 2 * jj)) % 4

    def pair_copy(jj, p):
        ja = (coord(me, p) + ahead(jj)) % 4
        other = 1 - core
        rows = pl.ds(8 * p, 8)
        if p == 0:
            src, dst = turned.at[:, :, ja, other, rows], turned_rx.at[:, :, ja, rows]
        elif p == 1:
            src, dst = turned.at[:, ja, :, other, rows], turned_rx.at[:, ja, :, rows]
        else:
            src, dst = turned.at[ja, :, :, other, rows], turned_rx.at[ja, :, :, rows]
        return remote(src, dst, small_sem.at[6], pair_recv.at[jj], partner)

    meta_copy = remote(meta.at[0], meta.at[1], sent.at[4], pair_recv.at[4], partner)

    def put_code(p, ja, jb, jc, lane0, v):
        codes2[p, ja, jb, jc, :, pl.ds(lane0, ROWS)] = jnp.concatenate([v, v - 1.0], axis=0).astype(BF16)

    def fill_own(m):
        m = (m + first) % LOADS
        z = m // 2
        for k in range(8):
            y, x = m % 2 * 2 + k // 4, k % 4
            for p in range(3):
                at = ((x, y, z), (y, z, x), (z, x, y))[p]
                put_code(p, *at, 0, turned[z, y, x, core, pl.ds(8 * p, 8), :])

    def fill_other(jj):
        for p in range(3):
            ja = (coord(me, p) + ahead(jj)) % 4
            for jb in range(4):
                for jc in range(4):
                    z, y, x = ((jc, jb, ja), (jb, ja, jc), (ja, jc, jb))[p]
                    put_code(p, ja, jb, jc, ROWS, turned_rx[z, y, x, pl.ds(8 * p, 8), :])

    def other_codes(jj):
        remote(turned_rx.at[0], turned_rx.at[0], small_sem.at[6], pair_recv.at[jj], partner).wait_recv()
        fill_other(jj)

    def turn(m):
        block = raw[m].astype(F32).astype(BF16)
        at = (m + first) % LOADS
        turned[at // 2, pl.ds(at % 2 * 2, 2)] = block.T.astype(F32).reshape(2, 4, 2, 24, ROWS)

    load(0).wait()
    turn(0)

    @pl.loop(1, LOADS)
    def _(m):
        load(m).wait()
        fill_own(m - 1)
        turn(m)

        @pl.when(m == 2)
        def _():
            pl.semaphore_wait(barrier, 10)
            pair_copy(0, 2).start()

    for p in range(2):
        pair_copy(0, p).start()

    @pl.loop(0, FEATS // 128)
    def _(k):
        pltpu.make_async_copy(cut_hbm.at[:, pl.ds(k * 128, 128)], cuts.at[k], load_sem.at[5]).start()

    fill_own(LOADS - 1)

    for one in small:
        one.wait()

    def goes_right(j):
        feat = feat_ref[j]
        owner = lax.div(feat, 24)
        bits = [lax.shift_right_logical(owner, k) for k in (5, 3, 1, 0)]
        column = turned[bits[0], bits[1] & 3, bits[2] & 3, bits[3] & 1, pl.ds(feat - 24 * owner, 1), :]
        return (column > thr_ref[j].astype(F32)).astype(jnp.int32)

    leaf = goes_right(0)
    for level in range(1, 5):
        width = 2 ** level
        bit = goes_right(width - 1)
        for n in range(1, width):
            bit = jnp.where(leaf == n, goes_right(width - 1 + n), bit)
        leaf = 2 * leaf + bit
    live = lax.broadcasted_iota(jnp.int32, (1, ROWS), 1) < valid_ref[...]
    grad = jnp.where(live, grad_ref[...], 0.0)
    hess = jnp.where(live, hess_ref[...], 0.0)
    meta[0] = jnp.concatenate([grad, hess, leaf.astype(F32), jnp.zeros((5, ROWS), F32)], axis=0)
    meta_copy.start()
    for jj in range(1, 4):
        for p in range(3):
            pair_copy(jj, p).start()

    def split3(v):
        hi = v.astype(BF16).astype(F32)
        mid = (v - hi).astype(BF16).astype(F32)
        return hi, mid, v - hi - mid

    def fill_weights(side):
        for k in range(ROWS // 128):
            lanes = pl.ds(k * 128, 128)
            g3 = split3(meta[side, 0:1, lanes])
            h3 = split3(meta[side, 1:2, lanes])
            hit = meta[side, 2:3, lanes] == lax.broadcasted_iota(jnp.int32, (LEAVES, 128), 0).astype(F32)
            rows = []
            for i in range(3):
                rows.append(jnp.where(hit, g3[i], 0.0))
                rows.append(jnp.where(hit, h3[i], 0.0))
            rows.append(jnp.zeros((64, 128), F32))
            weights[pl.ds(side * ROWS + k * 128, 128), :] = jnp.concatenate(rows, axis=0).T.astype(BF16)

    fill_weights(0)

    def block(ph, c, p, half, j):
        if ph == 0:
            return hist.at[p, c, j, half]
        return hist.at[p, c, coord(me, p), half, j]

    landings = (rx1, rx2)

    def copy(ph, c, p, kind, half):
        dim = (p + ph) % 3
        at = coord(me, dim)
        step = 1 if (kind == 1) == (half == 1) else -1
        j = (at + 2) % 4 if kind == 0 else (at + step + 4) % 4
        s = (ph * 2 + c) * 2 + (0 if kind == 0 else 1)
        return remote(block(ph, c, p, half, j), landings[ph].at[p, c, kind, half], sent.at[ph], recv_sem.at[s], neighbour(me, dim, step))

    def wait_landed(ph, c, p, kind, count):
        if p == 0:
            place = landings[ph].at[:, c, pl.ds(kind, count)]
            remote(place, place, sent.at[ph], recv_sem.at[(ph * 2 + c) * 2 + (0 if kind == 0 else 1)], partner).wait_recv()

    def send_far(ph, c, p):
        copy(ph, c, p, 0, 0).start()
        copy(ph, c, p, 0, 1).start()

    def send_near(ph, c, p):
        copy(ph, c, p, 1, 1).start()
        copy(ph, c, p, 1, 0).start()

    def relay(ph, c, p):
        at = coord(me, (p + ph) % 3)
        wait_landed(ph, c, p, 0, 1)
        for half in range(2):
            mine = block(ph, c, p, half, (at + (1, 3)[half]) % 4)
            mine[...] = mine[...] + landings[ph][p, c, 0, half]
            copy(ph, c, p, 2, half).start()

    def collect(ph, c, p):
        at = coord(me, (p + ph) % 3)
        wait_landed(ph, c, p, 1, 2)
        for half in range(2):
            mine = block(ph, c, p, half, at)
            total = mine[...] + landings[ph][p, c, 1, half] + landings[ph][p, c, 2, half]
            mine[...] = total
        if ph == 0:
            send_far(1, c, p)
            send_near(1, c, p)
        else:
            for step in (2, 1, 3):
                last_copy(c, p, step).start()

    def last_block(c, p, j):
        return hist.at[p, c, coord(me, p), :, coord(me, (p + 1) % 3), pl.ds(2 * j, 2)]

    def last_copy(c, p, step):
        dim = (p + 2) % 3
        j = (coord(me, dim) + step) % 4
        return remote(last_block(c, p, j), rx3.at[p, c, step - 1], sent.at[2], recv_sem.at[8 + c], neighbour(me, dim, step))

    def last_collect(c, p):
        if p == 0:
            remote(rx3.at[:, c], rx3.at[:, c], sent.at[2], recv_sem.at[8 + c], partner).wait_recv()
        out_ref[p, c] = last_block(c, p, coord(me, (p + 2) % 3))[...] + rx3[p, c, 0] + rx3[p, c, 1] + rx3[p, c, 2]

    first_half = lax.broadcasted_iota(jnp.int32, (64, 8, 128), 2) < 64

    def unit(c, p, jj, lane0, lanes, add):
        ja = (coord(me, p) + ahead(jj)) % 4
        bounds = [jnp.full((16, lanes), (8 * c + 2 * k).astype(F32), F32).astype(BF16) for k in range(4)]
        one = jnp.asarray(1, BF16)
        zero = jnp.asarray(0, BF16)
        pieces = []
        for half in range(2):
            for jb in range(4):
                for jc in range(4):
                    code = codes2[p, ja, jb, jc, :, pl.ds(lane0, lanes)]
                    for q in range(2):
                        pieces.append(jnp.where(code <= bounds[half * 2 + q], one, zero))
        left = jnp.concatenate(pieces, axis=0)
        sums = jnp.dot(left, weights[pl.ds(lane0, lanes), :], preferred_element_type=F32)
        sums = (sums[:, :128] + sums[:, 128:]).reshape(64, 2, 8, 128)
        even, odd = sums[:, 0], sums[:, 1]
        keep = jnp.where(first_half, even, odd)
        turn = jnp.where(first_half, odd, even).reshape(512, 128)
        both = (keep + pltpu.roll(turn, 64, 1).reshape(64, 8, 128)).reshape(2, 4, 8, 8, 128)
        if add:
            both = both + hist[p, c, ja]
        hist[p, c, ja] = both

    @pl.loop(0, 1 + me // GROUP)
    def _(z):
        for p in range(3):
            unit(z, p, z, 0, ROWS, False)

    other_codes(0)
    meta_copy.wait_recv()
    fill_weights(1)

    def for_parts(task, *args):
        for p in range(3):
            task(*args, p)

    @pl.loop(0, 1 + me // GROUP)
    def _(z):
        for p in range(3):
            unit(z, p, z, ROWS, ROWS, True)

    for_parts(send_far, 0, 0)

    def pick(b, *values):
        return sum((b == k + 1).astype(jnp.int32) * v for k, v in enumerate(values))

    @pl.loop(1, 8)
    def _(b):
        item = (1 - core) * pick(b, 6, 4, 1, 2, 5, 7, 3) + core * pick(b, 4, 5, 6, 1, 2, 7, 3)
        fresh = (1 - core) * pick(b, 1, 0, 1, 0, 0, 1, 0) + core * pick(b, 0, 1, 1, 0, 0, 1, 0)
        c, jj = item // 4, item % 4

        @pl.when(fresh == 1)
        def _():
            other_codes(jj)

        for p in range(3):
            unit(c, p, jj, 0, 2 * ROWS, False)

        @pl.when(jj == 0)
        def _():
            for_parts(send_far, 0, c)

        @pl.when(jj == 1)
        def _():
            for p in range(3):
                copy(0, c, p, 1, 1).start()

        @pl.when(jj == 2)
        def _():
            for p in range(3):
                copy(0, c, p, 1, 0).start()

        @pl.when((core == 0) & (b == 4))
        def _():
            for_parts(relay, 0, 0)

        @pl.when((core == 0) & (b == 5))
        def _():
            for_parts(relay, 0, 1)

        @pl.when((core == 1) & (b == 6))
        def _():
            for_parts(relay, 0, 0)

    pltpu.make_async_copy(cuts, cuts, load_sem.at[5]).wait()
    lanes = lax.broadcasted_iota(jnp.int32, (1, 128), 1)
    steps = lax.broadcasted_iota(jnp.int32, (BINS - 1, 128), 0)
    value = jnp.zeros((1, 128), F32)
    for j in range(INNER):
        feat = feat_ref[j]
        one = jnp.sum(jnp.where(steps == thr_ref[j], cuts[feat // 128], 0.0), axis=0, keepdims=True)
        one = jnp.sum(jnp.where(lanes == feat % 128, one, 0.0), axis=1, keepdims=True)
        value = jnp.where(lanes == j, one, value)
    value_ref[...] = jnp.where(lanes == 127, reg_ref[...], value)

    @pl.when(core == 1)
    def _():
        for_parts(relay, 0, 1)

    for_parts(collect, 0, 0)
    for_parts(collect, 0, 1)
    for_parts(relay, 1, 0)
    for_parts(relay, 1, 1)
    for_parts(collect, 1, 0)
    for_parts(collect, 1, 1)
    for_parts(last_collect, 0)
    for_parts(last_collect, 1)

    meta_copy.wait_send()
    remote(turned_rx, turned_rx, small_sem.at[6], pair_recv.at[4], partner).wait_send()
    for ph, place in enumerate((rx1, rx2, rx3)):
        remote(place, place, sent.at[ph], recv_sem.at[0], partner).wait_send()


def gain_kernel(sums_ref, found_ref, gain_ref, leaf_ref, value_ref):
    reg = found_ref[0:1, 127:128]
    sums = sums_ref[...].reshape(192, 128)
    lane = lax.broadcasted_iota(jnp.int32, (128, 256), 0)
    col = lax.broadcasted_iota(jnp.int32, (128, 256), 1)
    same = (lane // 64 == col // 64 % 2) & (lane // 32 % 2 == col // 128)
    under = lane % 32 + 32
    hit = under == col % 64 + 1
    for _ in range(5):
        under = under // 2
        hit = hit | (under == col % 64 + 1)
    pick = jnp.where(same & hit, 1.0, 0.0).astype(BF16)
    hi = sums.astype(BF16)
    rest = sums - hi.astype(F32)
    mid = rest.astype(BF16)
    low = (rest - mid.astype(F32)).astype(BF16)
    nodes = jnp.dot(jnp.concatenate([low, mid, hi], axis=1), jnp.concatenate([pick] * 3, axis=0), preferred_element_type=F32)
    grad = nodes[:, :128].reshape(3, 8, 8, 128)
    hess = nodes[:, 128:].reshape(3, 8, 8, 128)
    upper = lax.broadcasted_iota(jnp.int32, (8, 128), 1) >= 64

    def score(g, h):
        return g * g / (h + reg)

    for p in range(3):
        g_all, h_all = grad[p, 7], hess[p, 7]
        g_all = jnp.where(upper, g_all, pltpu.roll(g_all, 64, 1))
        h_all = jnp.where(upper, h_all, pltpu.roll(h_all, 64, 1))
        whole = score(g_all, h_all)
        for q in range(8):
            g_left, h_left = grad[p, q], hess[p, q]
            gain = 0.5 * (score(g_left, h_left) + score(g_all - g_left, h_all - h_left) - whole)
            gain_ref[2 * q, pl.ds(8 * p, 8), :] = gain[:, :63]
            if q < 7:
                gain_ref[2 * q + 1, pl.ds(8 * p, 8), :] = pltpu.roll(gain, 64, 1)[:, :63]
    last = sums_ref[0, 1, 1, 1]
    g_leaf, h_leaf = pltpu.roll(last, 64, 1), pltpu.roll(last, 32, 1)
    leaf_ref[...] = (-g_leaf / (h_leaf + reg))[0:1, :LEAVES]
    value_ref[...] = found_ref[:, :INNER]


def solution(mesh):
    row_spec = P(('trees', 'data'))
    vmem = pl.BlockSpec(memory_space=pltpu.VMEM)
    hbm = pl.BlockSpec(memory_space=pl.ANY)

    def device_fn(bin_codes, gradient, hessian, valid_rows, split_feat, split_thr, cut_values, reg_lambda):
        sums, found = pl.pallas_call(
            hist_kernel,
            out_shape=(pltpu.VMEM((3, 2, 2, 2, 8, 128), F32), pltpu.VMEM((1, 128), F32)),
            in_specs=[hbm] * 8,
            out_specs=(vmem, vmem),
            scratch_shapes=[
                pltpu.VMEM((1, ROWS), F32),
                pltpu.VMEM((1, ROWS), F32),
                pltpu.VMEM((1, 1), jnp.int32),
                pltpu.SMEM((INNER,), jnp.int32),
                pltpu.SMEM((INNER,), jnp.int32),
                pltpu.VMEM((1, 1), F32),
                pltpu.VMEM((LOADS, ROWS, SLAB), jnp.int32),
                pltpu.VMEM((4, 4, 4, 2, 24, ROWS), F32),
                pltpu.VMEM((4, 4, 4, 24, ROWS), F32),
                pltpu.VMEM((3, 4, 4, 4, 16, 2 * ROWS), BF16),
                pltpu.VMEM((2, 8, ROWS), F32),
                pltpu.VMEM((2 * ROWS, 256), BF16),
                pltpu.VMEM((FEATS // 128, BINS - 1, 128), F32),
                pltpu.VMEM((3, 2, 4, 2, 4, 8, 8, 128), F32),
                pltpu.VMEM((3, 2, 3, 2, 4, 8, 8, 128), F32),
                pltpu.VMEM((3, 2, 3, 2, 8, 8, 128), F32),
                pltpu.VMEM((3, 2, 3, 2, 2, 8, 128), F32),
                pltpu.SemaphoreType.DMA((LOADS,)),
                pltpu.SemaphoreType.DMA((7,)),
                pltpu.SemaphoreType.DMA((5,)),
                pltpu.SemaphoreType.DMA((10,)),
            ],
            compiler_params=pltpu.CompilerParams(collective_id=0, has_side_effects=True, vmem_limit_bytes=60 * 1024 * 1024),
            name='hist',
        )(bin_codes, gradient.reshape(1, ROWS), hessian.reshape(1, ROWS), valid_rows.reshape(1, 1), split_feat, split_thr, cut_values.T, reg_lambda.reshape(1, 1))
        gain, leaf, value = pl.pallas_call(
            gain_kernel,
            out_shape=(jax.ShapeDtypeStruct((BINS - 1, FEATS // 128, 63), F32), jax.ShapeDtypeStruct((1, LEAVES), F32), jax.ShapeDtypeStruct((1, INNER), F32)),
            in_specs=[vmem, vmem],
            out_specs=(vmem, vmem, vmem),
            compiler_params=pltpu.CompilerParams(vmem_limit_bytes=4 * 1024 * 1024),
            name='gain',
        )(sums, found)
        return jnp.transpose(gain, (2, 1, 0)), leaf.reshape(LEAVES), value.reshape(INNER)

    return jax.shard_map(device_fn, mesh=mesh, in_specs=(P(('trees', 'data'), None), row_spec, row_spec, row_spec, P('trees'), P('trees'), P('trees', None), P('trees')), out_specs=(P(None, ('trees', 'data'), None), P('trees'), P('trees')), check_vma=False)
```
